32 devices in a mesh: groups: 2 (over x), ctx: 16 (over z, y, core).
Axes of the slice: x: 2, y: 2, z: 4, core: 2. Of those that a mesh axis runs over, the one named last changes fastest.
Arguments:
- query_states: bfloat16 [16384, 32, 128], P(('groups', 'ctx')), parts along dimension 0, may hold values from -20 to 20
- key_states: bfloat16 [16384, 8, 128], P(('groups', 'ctx')), parts along dimension 0, may hold values from -4 to 4
- value_states: bfloat16 [16384, 8, 128], P(('groups', 'ctx')), parts along dimension 0, may hold values from -6 to 6
- vert_blocks: int32 [16, 4], P('groups'), parts along dimension 0, may hold values from 0 to 63, as said below
- vert_count: int32 [16], P('groups'), parts along dimension 0, may hold values from 1 to 4, as said below
- slash_offsets: int32 [16, 4], P('groups'), parts along dimension 0, may hold values from 0 to 8, as said below
- slash_count: int32 [16], P('groups'), parts along dimension 0, may hold values from 1 to 4, as said below
Outputs:
- attended: bfloat16 [16384, 32, 128], P(('groups', 'ctx')), parts along dimension 0
The draws below stay inside these ranges and needn't reach their ends.
There are 2 independent parts, one for each index of `groups`. The reference program is written for one: setup_inputs(seed, part) draws one part's arguments, and reference() takes and returns one part's arrays. A program takes and returns all parts, laid end to end along the dimension named above; each array names one. Nothing has to cross between parts.
Inputs may be any that keep to these rules, and one draw needn't show every extreme that they name: `vert_blocks`: the 4 entries of each head are distinct; in some head the first entry lies in one of the first 4 blocks. `vert_count`: some head uses all 4 entries. `slash_offsets`: the 4 entries of each head are distinct and the first is 0. `slash_count`: some head uses all 4 entries.
All inputs are finite; a program needn't handle non-finite values.
Results may differ from the reference program's by a relative error of at most 0.0048.
Values may be sent and summed in bfloat16 or wider, within the bound.
A program may use at most 128 MiB of HBM per device.

```python
import math
import jax
import jax.numpy as jnp
from jax import lax

QH = 32
KVH = 8
DH = 128
BLOCK = 128
NV = 4
NS = 4
SEQ_DEV = 512
TOKENS = 8192
NBLK = 64


def draw_query_states(key, part):
    base = jnp.clip(jax.random.normal(jax.random.fold_in(key, 11), (TOKENS, QH, DH), jnp.float32), -4.0, 4.0)
    return base.astype(jnp.bfloat16)


def draw_key_states(key, part):
    base = jnp.clip(jax.random.normal(jax.random.fold_in(key, 12), (TOKENS, KVH, DH), jnp.float32), -4.0, 4.0)
    return base.astype(jnp.bfloat16)


def draw_vert_blocks(key, part):
    head_keys = jax.random.split(jax.random.fold_in(key, 21), KVH)
    picked = jax.vmap(lambda one_key: jax.random.permutation(one_key, NBLK)[:NV])(head_keys).astype(jnp.int32)
    first_dev = SEQ_DEV // BLOCK
    lowest = jax.random.randint(jax.random.fold_in(key, 22), (), 0, first_dev).astype(jnp.int32)
    others = jax.random.permutation(jax.random.fold_in(key, 23), NBLK - 1)[:NV - 1].astype(jnp.int32)
    others = others + (others >= lowest).astype(jnp.int32)
    special = jnp.concatenate((lowest[None], others))
    chosen = jax.random.randint(jax.random.fold_in(key, 24), (), 0, KVH)
    picked = jnp.where((jnp.arange(KVH) == chosen)[:, None], special[None, :], picked)
    return picked.astype(jnp.int32)


def draw_vert_count(key, part):
    counts = jax.random.randint(jax.random.fold_in(key, 31), (KVH,), 1, NV + 1)
    fullest = jax.random.randint(jax.random.fold_in(key, 32), (), 0, KVH)
    return counts.at[fullest].set(NV).astype(jnp.int32)


def draw_slash_offsets(key, part):
    head_keys = jax.random.split(jax.random.fold_in(key, 41), KVH)
    reach = 2 * (SEQ_DEV // BLOCK)
    others = jax.vmap(lambda one_key: jax.random.permutation(one_key, reach)[:NS - 1] + 1)(head_keys)
    return jnp.concatenate((jnp.zeros((KVH, 1), jnp.int32), others.astype(jnp.int32)), axis=1)


def draw_slash_count(key, part):
    counts = jax.random.randint(jax.random.fold_in(key, 51), (KVH,), 1, NS + 1)
    fullest = jax.random.randint(jax.random.fold_in(key, 52), (), 0, KVH)
    return counts.at[fullest].set(NS).astype(jnp.int32)


def block_scale(rng, shape, cuts, low, largest):
    def one(position, blocks):
        draws = jax.random.uniform(jax.random.fold_in(jax.random.fold_in(rng, 6), position), (blocks,), jnp.float32, low / len(cuts), largest / len(cuts))
        return jnp.repeat(jnp.exp(draws), shape[position] // blocks).reshape((-1,) + (1,) * (len(shape) - position - 1))

    gain = one(*cuts[0])
    for cut in cuts[1:]:
        gain = gain * one(*cut)
    return gain


def centred(key, dims, deviation, bound, pieces=(), kind=jnp.bfloat16):
    entries = deviation * jax.random.normal(key, dims, jnp.float32)
    if pieces:
        entries = entries * block_scale(key, dims, pieces, -0.22, 0.18)
    return jnp.clip(entries, -bound, bound).astype(kind)


def setup_inputs(seed: int = 0, part: int = 0) -> dict:
    key_of = jax.random.split(jax.random.key(seed), 8)
    part_keys = jax.random.split(jax.random.fold_in(key_of[7], part), 8)
    query_states = draw_query_states(jax.random.fold_in(jax.random.fold_in(key_of[7], part), 71), part)
    key_states = draw_key_states(jax.random.fold_in(jax.random.fold_in(key_of[7], part), 71), part)
    value_states = centred(part_keys[2], (TOKENS, KVH, DH), 1.0, 6.0, ((0, 16),))
    vert_blocks = draw_vert_blocks(jax.random.fold_in(jax.random.fold_in(key_of[7], part), 71), part)
    vert_count = draw_vert_count(jax.random.fold_in(jax.random.fold_in(key_of[7], part), 71), part)
    slash_offsets = draw_slash_offsets(jax.random.fold_in(jax.random.fold_in(key_of[7], part), 71), part)
    slash_count = draw_slash_count(jax.random.fold_in(jax.random.fold_in(key_of[7], part), 71), part)
    return dict(query_states=query_states, key_states=key_states, value_states=value_states, vert_blocks=vert_blocks, vert_count=vert_count, slash_offsets=slash_offsets, slash_count=slash_count)


def reference(query_states, key_states, value_states, vert_blocks, vert_count, slash_offsets, slash_count):
    group_size = QH // KVH
    key_tiles_all = key_states.reshape(NBLK, BLOCK, KVH, DH)
    value_tiles_all = value_states.reshape(NBLK, BLOCK, KVH, DH)
    head_ids = jnp.arange(KVH, dtype=jnp.int32)
    vert_slot = jnp.arange(NV, dtype=jnp.int32)[None, :] < vert_count[:, None]
    slash_slot = jnp.arange(NS, dtype=jnp.int32)[None, :] < slash_count[:, None]
    inv_root = 1.0 / math.sqrt(DH)
    within = jnp.arange(BLOCK, dtype=jnp.int32)

    def query_block(qblock):
        slash_blocks = qblock - slash_offsets
        repeated = jnp.any(vert_slot[:, None, :] & (vert_blocks[:, None, :] == slash_blocks[:, :, None]), axis=-1)
        slash_ok = slash_slot & (slash_blocks >= 0) & jnp.logical_not(repeated)
        vert_ok = vert_slot & (vert_blocks <= qblock)
        key_blocks = jnp.concatenate((vert_blocks, slash_blocks), axis=1)
        usable = jnp.concatenate((vert_ok, slash_ok), axis=1)
        clipped = jnp.clip(key_blocks, 0, NBLK - 1)
        key_tiles = key_tiles_all[clipped, :, head_ids[:, None], :]
        value_tiles = value_tiles_all[clipped, :, head_ids[:, None], :]
        query_rows = lax.dynamic_slice_in_dim(query_states, qblock * BLOCK, BLOCK, 0).reshape(BLOCK, KVH, group_size, DH)
        scores = jnp.einsum('qgrd,gntd->grqnt', query_rows.astype(jnp.float32), key_tiles.astype(jnp.float32)) * inv_root
        scores = scores.reshape(KVH, group_size, BLOCK, (NV + NS) * BLOCK)
        key_pos = (key_blocks[:, :, None] * BLOCK + within[None, None, :]).reshape(KVH, (NV + NS) * BLOCK)
        query_pos = qblock * BLOCK + within
        allowed = jnp.repeat(usable, BLOCK, axis=1)[:, None, :] & (key_pos[:, None, :] <= query_pos[None, :, None])
        allowed = allowed[:, None, :, :]
        masked = jnp.where(allowed, scores, -1e+30)
        row_max = lax.optimization_barrier(jnp.max(masked, axis=-1, keepdims=True))
        powers = jnp.where(allowed, jnp.exp(masked - row_max), 0.0)
        weights = (powers / lax.optimization_barrier(jnp.sum(powers, axis=-1, keepdims=True))).astype(jnp.bfloat16)
        values_flat = value_tiles.reshape(KVH, (NV + NS) * BLOCK, DH).astype(jnp.float32)
        result = jnp.einsum('grqk,gkd->qgrd', weights.astype(jnp.float32), values_flat)
        return result.reshape(BLOCK, QH, DH).astype(jnp.bfloat16)
    blocks = lax.map(query_block, jnp.arange(NBLK, dtype=jnp.int32))
    return blocks.reshape(TOKENS, QH, DH)
```

```python
import functools
import math

import jax
import jax.numpy as jnp
from jax import lax
from jax.experimental import pallas as pl
from jax.experimental.pallas import tpu as pltpu
from jax.sharding import PartitionSpec as P

BLOCK = 128
LARGEST_OFFSET = 8
MASKED = -1e30


def attend_head(head, dims, device, tables, q_ref, window, columns, diagonal, unit, out_ref):
    per_dev, reach, n_vert, n_slash, group_size, head_dim = dims
    vb_ref, vc_ref, so_ref, sc_ref = tables
    scale = math.log2(math.e) / math.sqrt(head_dim)
    n_tiles = n_vert + n_slash
    chunk = 2 if group_size % 2 == 0 else 1
    parts = group_size // chunk

    def one_block(block, carry):
        qblock = device * per_dev + block
        start = pl.multiple_of(block * BLOCK, BLOCK)
        own = reach * per_dev + block
        spots, usable = [own], []
        for s in range(1, n_slash):
            offset = so_ref[head, s]
            ok = (s < sc_ref[head]) & (offset <= qblock)
            for v in range(n_vert):
                ok = ok & ((v >= vc_ref[head]) | (vb_ref[head, v] != qblock - offset))
            usable.append(ok)
            spots.append(jnp.where(ok, own - offset, own))
        for v in range(n_vert):
            usable.append((v < vc_ref[head]) & (vb_ref[head, v] < qblock))
        keys = [window[spot, 0] for spot in spots]
        values = [window[spot, 1] for spot in spots]
        for v in range(n_vert):
            row = (head * n_vert + v) * 2 * BLOCK
            keys.append(columns[row : row + BLOCK, :])
            values.append(columns[row + BLOCK : row + 2 * BLOCK, :])
        masks = [diagonal[...]]
        for ok in usable:
            fill = jnp.where(ok, 0.0, MASKED).astype(jnp.float32)
            masks.append(jnp.full((BLOCK, BLOCK), fill, jnp.float32).astype(jnp.bfloat16))
        keys = jnp.concatenate(
            [jnp.concatenate(keys, axis=0), jnp.concatenate(masks, axis=0)], axis=1
        )
        ones = jnp.ones((n_tiles * BLOCK, head_dim), jnp.bfloat16)
        values = jnp.concatenate([jnp.concatenate(values, axis=0), ones], axis=1)

        def scores_of(part):
            queries = []
            for h in range(part * chunk, (part + 1) * chunk):
                lane = (head * group_size + h) * head_dim
                rows = q_ref[pl.ds(start, BLOCK), lane : lane + head_dim]
                queries.append(jnp.concatenate([rows, unit[...]], axis=1))
            tile = lax.dot_general(
                jnp.concatenate(queries, axis=0), keys, (((1,), (1,)), ((), ())),
                preferred_element_type=jnp.float32,
            )
            return [tile[:, i * BLOCK : (i + 1) * BLOCK] for i in range(n_tiles)]

        def top_of(scores):
            return jnp.max(functools.reduce(jnp.maximum, scores), axis=1, keepdims=True) * scale

        def sums_of(scores, top):
            powers = [jnp.exp2(tile * scale - top).astype(jnp.bfloat16) for tile in scores]
            return jnp.dot(
                jnp.concatenate(powers, axis=1), values, preferred_element_type=jnp.float32
            )

        def store(part, sums):
            result = (sums[:, :head_dim] / sums[:, head_dim:]).astype(jnp.bfloat16)
            for i in range(chunk):
                lane = (head * group_size + part * chunk + i) * head_dim
                out_ref[pl.ds(start, BLOCK), lane : lane + head_dim] = result[
                    i * BLOCK : (i + 1) * BLOCK
                ]

        scores = scores_of(0)
        top = top_of(scores)
        last = None
        for part in range(parts):
            following = scores_of(part + 1) if part + 1 < parts else None
            sums = sums_of(scores, top)
            if following is not None:
                top = top_of(following)
            if last is not None:
                store(part - 1, last)
            scores, last = following, sums
        store(parts - 1, last)
        return carry

    lax.fori_loop(0, per_dev, one_block, 0)


def fused_kernel(
    size, kv_heads, relayed, dims,
    vb_ref, vc_ref, so_ref, sc_ref, own_ref, q_ref, out_ref,
    acc, landed, full, stage, diagonal, unit, *scratch,
):
    per_dev, reach, n_vert, n_slash, group_size, head_dim = dims
    windows = scratch[:kv_heads]
    (
        fold_send, fold_recv, grow_send, grow_recv, far_send, far_recv,
        near_send, near_recv, pass_send, pass_recv,
    ) = scratch[kv_heads:]
    tables = (vb_ref, vc_ref, so_ref, sc_ref)
    device = lax.axis_index("ctx")
    odd = lax.rem(device, 2)
    side = lax.rem(device // 2, 2)
    line = device // 4
    line_bits = size.bit_length() - 3
    direct = kv_heads - relayed

    def remote(src, dst, send, recv, target):
        return pltpu.make_async_remote_copy(
            src_ref=src, dst_ref=dst, send_sem=send, recv_sem=recv,
            device_id={"ctx": target}, device_id_type=pl.DeviceIdType.MESH,
        )

    def when(condition):
        return pl.when(condition)

    last = size - 1
    sends_far = device + reach < size
    gets_far = device >= reach
    crossing = (side == 1) & sends_far
    passes = (side == 0) & (device + 2 * reach < size)
    gets_passed = (side == 0) & gets_far
    partner = device + 1 - 2 * odd

    masks, bits = [], []
    gray = line ^ (line // 2)
    for j in range(line_bits):
        k, r = j, line_bits - 1 - j
        masks.append(jnp.where(odd == 0, 4 * ((2 << k) - 1), 4 * ((2 << r) - 1)))
        bits.append(jnp.where(odd == 0, lax.rem(gray // (1 << k), 2), lax.rem(gray // (1 << r), 2)))
    partners = [partner] + [device ^ mask for mask in masks]
    bits = [odd] + bits
    across = device ^ 2
    rounds = len(partners)

    barrier = pltpu.get_barrier_semaphore()

    def greet(target):
        pl.semaphore_signal(
            barrier, inc=1, device_id={"ctx": target}, device_id_type=pl.DeviceIdType.MESH
        )

    for target in partners + [across]:
        greet(target)
    for condition, target in (
        (crossing, device + reach), (gets_passed, device - reach),
        (passes, device + 2 * reach), (gets_passed & (device >= 2 * reach), device - 2 * reach),
    ):
        @when(condition)
        def _(target=target):
            greet(target)

    rows_i = lax.broadcasted_iota(jnp.int32, (BLOCK, BLOCK), 0)
    cols_i = lax.broadcasted_iota(jnp.int32, (BLOCK, BLOCK), 1)
    diagonal[...] = jnp.where(cols_i >= rows_i, 0.0, MASKED).astype(jnp.bfloat16)
    unit[...] = jnp.where(rows_i == cols_i, 1.0, 0.0).astype(jnp.bfloat16)

    def one_head(head, carry):
        for v in range(n_vert):
            at = vb_ref[head, v] - device * per_dev
            mine = (v < vc_ref[head]) & (at >= 0) & (at < per_dev)
            at = jnp.clip(at, 0, per_dev - 1)
            for kv in range(2):
                tile = own_ref[head, at, kv].astype(jnp.float32)
                row = pl.multiple_of(((head * n_vert + v) * 2 + kv) * BLOCK, BLOCK)
                acc[pl.ds(row, BLOCK), :] = jnp.where(mine, tile, 0.0).astype(jnp.bfloat16)
        return carry

    lax.fori_loop(0, kv_heads, one_head, 0)
    for head in range(kv_heads):
        windows[head][reach * per_dev : (reach + 1) * per_dev] = own_ref[head]

    arrivals = jnp.int32(rounds + 1)
    for condition in (crossing, gets_passed, passes, gets_passed & (device >= 2 * reach)):
        arrivals = arrivals + condition.astype(jnp.int32)
    pl.semaphore_wait(barrier, arrivals)

    def place(head, where):
        return windows[head].at[pl.ds(where * per_dev, per_dev)]

    def far_copy(head):
        target = jnp.minimum(device + reach, last)
        return remote(own_ref.at[head], place(head, 0), far_send.at[head], far_recv.at[head], target)

    def stage_copy(head):
        slot = stage.at[head - direct]
        target = jnp.maximum(device - reach, 0)
        return remote(own_ref.at[head], slot, far_send.at[head], pass_recv.at[head - direct], target)

    def pass_copy(head):
        slot = stage.at[head - direct]
        target = jnp.minimum(device + 2 * reach, last)
        return remote(
            slot, place(head, 0), pass_send.at[head - direct], far_recv.at[head], target
        )

    def near_copy(head):
        return remote(
            own_ref.at[head], place(head, 1), near_send.at[head], near_recv.at[head], partner
        )

    def relay_copy(head):
        return remote(
            place(head, 0), place(head, 1), near_send.at[head], near_recv.at[head], partner
        )

    def start_far(condition, heads):
        @when(condition)
        def _():
            for head in heads:
                far_copy(head).start()

    total_rows = kv_heads * n_vert * 2 * BLOCK
    base, length, offset = jnp.int32(0), total_rows, 0
    bases, folds = [], []

    def fold(k):
        half = length // 2
        kept = pl.multiple_of(base + bits[k] * half, 16)
        given = pl.multiple_of(base + (1 - bits[k]) * half, 16)
        copy = remote(
            acc.at[pl.ds(given, half)], landed.at[pl.ds(offset, half)],
            fold_send.at[k], fold_recv.at[k], partners[k],
        )
        copy.start()
        return copy, kept, half

    def add(dst, kept, offset, rows):
        step = min(rows, 256)

        def body(i, carry):
            here = pl.ds(pl.multiple_of(kept + i * step, 16), step)
            there = pl.ds(pl.multiple_of(offset + i * step, 16), step)
            dst[here, :] = acc[here, :] + landed[there, :]
            return carry

        lax.fori_loop(0, rows // step, body, 0)

    early = 3 * kv_heads // 8
    for k in range(rounds):
        copy, kept, half = fold(k)
        folds.append(copy)
        if k == 0:
            start_far(side == 0, range(early))

            @when(crossing)
            def _():
                for head in range(direct, kv_heads):
                    stage_copy(head).start()

            @when(odd == 0)
            def _():
                for head in range(kv_heads):
                    near_copy(head).start()

        if k == rounds - 1:
            start_far(crossing, range(min(2, direct)))
        copy.wait_recv()
        add(acc, kept, offset, half)
        bases.append(kept)
        base, length, offset = kept, half, offset + half

    swap = remote(
        acc.at[pl.ds(base, length)], landed.at[pl.ds(offset, length)],
        fold_send.at[rounds], fold_recv.at[rounds], across,
    )
    swap.start()
    start_far(side == 0, range(early, kv_heads))
    swap.wait_recv()
    add(full, base, offset, length)
    folds.append(swap)

    grows = []
    for k in reversed(range(rounds)):
        part = pl.ds(bases[k], total_rows >> (k + 1))
        copy = remote(full.at[part], full.at[part], grow_send.at[k], grow_recv.at[k], partners[k])
        copy.start()
        grows.append(copy)
        if k == min(1, rounds - 1):
            start_far(crossing, range(min(2, direct), direct))

            @when(passes)
            def _():
                for head in range(direct, kv_heads):
                    stage_copy(head).wait_recv()
                    pass_copy(head).start()

        copy.wait_recv()

    for head in range(kv_heads):
        @when(gets_far)
        def _():
            far_copy(head).wait_recv()

            @when(odd == 1)
            def _():
                relay_copy(head).start()

        @when((odd == 1) | gets_far)
        def _():
            near_copy(head).wait_recv()

        attend_head(
            head, dims, device, tables, q_ref, windows[head], full, diagonal, unit, out_ref
        )

    @when(sends_far)
    def _():
        for head in range(kv_heads):
            far_copy(head).wait_send()

    @when((odd == 0) | gets_far)
    def _():
        for head in range(kv_heads):
            near_copy(head).wait_send()

    @when(passes)
    def _():
        for head in range(direct, kv_heads):
            pass_copy(head).wait_send()

    for copy in folds + grows:
        copy.wait_send()


def fused(own, queries, vert_blocks, vert_count, slash_offsets, slash_count, group_size):
    size = lax.axis_size("ctx")
    kv_heads, per_dev, _, _, head_dim = own.shape
    n_vert = vert_blocks.shape[1]
    n_slash = slash_offsets.shape[1]
    reach = -(-LARGEST_OFFSET // per_dev)
    relayed = 3 * kv_heads // 8
    rounds = size.bit_length() - 2
    dims = (per_dev, reach, n_vert, n_slash, group_size, head_dim)
    dma = pltpu.SemaphoreType.DMA
    columns = pltpu.VMEM((kv_heads * n_vert * 2 * BLOCK, head_dim), own.dtype)
    square = pltpu.VMEM((BLOCK, BLOCK), own.dtype)
    window = pltpu.VMEM(((reach + 1) * per_dev, 2, BLOCK, head_dim), own.dtype)
    smem = pl.BlockSpec(memory_space=pltpu.SMEM)
    vmem = pl.BlockSpec(memory_space=pltpu.VMEM)
    return pl.pallas_call(
        functools.partial(fused_kernel, size, kv_heads, relayed, dims),
        out_shape=jax.ShapeDtypeStruct(queries.shape, queries.dtype),
        in_specs=[smem] * 4 + [vmem] * 2,
        out_specs=vmem,
        scratch_shapes=[columns] * 3
        + [pltpu.VMEM((relayed, per_dev, 2, BLOCK, head_dim), own.dtype)]
        + [square] * 2
        + [window] * kv_heads
        + [dma((rounds + 1,))] * 2
        + [dma((rounds,))] * 2
        + [dma((kv_heads,))] * 4
        + [dma((relayed,))] * 2,
        compiler_params=pltpu.CompilerParams(
            collective_id=0, has_side_effects=True, vmem_limit_bytes=56 * 1024 * 1024
        ),
        name="fused",
    )(vert_blocks, vert_count, slash_offsets, slash_count, own, queries)


def local(
    query_states, key_states, value_states, vert_blocks, vert_count, slash_offsets, slash_count
):
    rows_dev, q_heads, head_dim = query_states.shape
    kv_heads = key_states.shape[1]
    group_size = q_heads // kv_heads
    per_dev = rows_dev // BLOCK

    def by_tile(x):
        return jnp.transpose(x.reshape(per_dev, BLOCK, kv_heads, head_dim), (2, 0, 1, 3))

    own = jnp.stack((by_tile(key_states), by_tile(value_states)), axis=2)
    out = fused(
        own,
        query_states.reshape(rows_dev, q_heads * head_dim),
        vert_blocks,
        vert_count,
        slash_offsets,
        slash_count,
        group_size,
    )
    return out.reshape(rows_dev, q_heads, head_dim)


def solution(mesh):
    in_specs = (
        P(("groups", "ctx"), None, None),
        P(("groups", "ctx"), None, None),
        P(("groups", "ctx"), None, None),
        P("groups", None),
        P("groups"),
        P("groups", None),
        P("groups"),
    )
    out_specs = P(("groups", "ctx"), None, None)
    return jax.shard_map(local, mesh=mesh, in_specs=in_specs, out_specs=out_specs, check_vma=False)
```

```python
import functools
import math

import jax
import jax.numpy as jnp
from jax import lax
from jax.experimental import pallas as pl
from jax.experimental.pallas import tpu as pltpu
from jax.sharding import PartitionSpec as P

BLOCK = 128
LARGEST_OFFSET = 8
MASKED = -1e30
CHUNKS = 2


def attend_head(head, dims, device, tables, q_ref, window, columns, diagonal, unit, out_ref):
    per_dev, reach, n_vert, n_slash, group_size, head_dim = dims
    vb_ref, vc_ref, so_ref, sc_ref = tables
    scale = math.log2(math.e) / math.sqrt(head_dim)
    n_tiles = n_vert + n_slash
    chunk = 2 if group_size % 2 == 0 else 1
    parts = group_size // chunk

    def one_block(block, carry):
        qblock = device * per_dev + block
        start = pl.multiple_of(block * BLOCK, BLOCK)
        own = reach * per_dev + block
        spots, usable = [own], []
        for s in range(1, n_slash):
            offset = so_ref[s, head]
            ok = (s < sc_ref[head]) & (offset <= qblock)
            for v in range(n_vert):
                ok = ok & ((v >= vc_ref[head]) | (vb_ref[v, head] != qblock - offset))
            usable.append(ok)
            spots.append(jnp.where(ok, own - offset, own))
        for v in range(n_vert):
            usable.append((v < vc_ref[head]) & (vb_ref[v, head] < qblock))
        keys = [window[spot, 0] for spot in spots]
        values = [window[spot, 1] for spot in spots]
        for v in range(n_vert):
            row = (head * n_vert + v) * 2 * BLOCK
            keys.append(columns[row : row + BLOCK, :])
            values.append(columns[row + BLOCK : row + 2 * BLOCK, :])
        masks = [diagonal[...]]
        for ok in usable:
            fill = jnp.where(ok, 0.0, MASKED).astype(jnp.float32)
            masks.append(jnp.full((BLOCK, BLOCK), fill, jnp.float32).astype(jnp.bfloat16))
        keys = jnp.concatenate(
            [jnp.concatenate(keys, axis=0), jnp.concatenate(masks, axis=0)], axis=1
        )
        values = jnp.concatenate(values, axis=0)

        def scores_of(part):
            queries = []
            for h in range(part * chunk, (part + 1) * chunk):
                lane = (head * group_size + h) * head_dim
                rows = q_ref[pl.ds(start, BLOCK), lane : lane + head_dim]
                queries.append(jnp.concatenate([rows, unit[...]], axis=1))
            tile = lax.dot_general(
                jnp.concatenate(queries, axis=0), keys, (((1,), (1,)), ((), ())),
                preferred_element_type=jnp.float32,
            )
            return [tile[:, i * BLOCK : (i + 1) * BLOCK] for i in range(n_tiles)]

        def top_of(scores):
            return jnp.max(functools.reduce(jnp.maximum, scores), axis=1, keepdims=True)

        def sums_of(scores, top):
            powers = [jnp.exp2((tile - top) * scale) for tile in scores]
            total = jnp.sum(functools.reduce(jnp.add, powers), axis=1, keepdims=True)
            weights = jnp.concatenate([p.astype(jnp.bfloat16) for p in powers], axis=1)
            return jnp.dot(weights, values, preferred_element_type=jnp.float32), total

        def store(part, sums):
            result = (sums[0] / sums[1]).astype(jnp.bfloat16)
            for i in range(chunk):
                lane = (head * group_size + part * chunk + i) * head_dim
                out_ref[pl.ds(start, BLOCK), lane : lane + head_dim] = result[
                    i * BLOCK : (i + 1) * BLOCK
                ]

        scores = scores_of(0)
        top = top_of(scores)
        last = None
        for part in range(parts):
            following = scores_of(part + 1) if part + 1 < parts else None
            sums = sums_of(scores, top)
            if following is not None:
                top = top_of(following)
            if last is not None:
                store(part - 1, last)
            scores, last = following, sums
        store(parts - 1, last)
        return carry

    lax.fori_loop(0, per_dev, one_block, 0, unroll=2 if per_dev % 2 == 0 else 1)


def fused_kernel(
    size, kv_heads, relayed, dims,
    vb_ref, vc_ref, so_ref, sc_ref, k_ref, v_ref, q_ref, out_ref,
    own_ref, qs_ref, acc, landed, full, stage, diagonal, unit, *scratch,
):
    per_dev, reach, n_vert, n_slash, group_size, head_dim = dims
    windows = scratch[:kv_heads]
    (
        core_send, core_recv, grow_send, grow_recv, swap_send, swap_recv,
        up_recv, down_recv, line_send, spread_recv, above_send, below_send,
        far_send, far_recv, near_send, near_recv, pass_send, pass_recv,
    ) = scratch[kv_heads:]
    tables = (vb_ref, vc_ref, so_ref, sc_ref)
    device = lax.axis_index("ctx")
    odd = lax.rem(device, 2)
    side = lax.rem(device // 2, 2)
    line = device // 4
    length = size // 4
    direct = kv_heads - relayed
    last = size - 1

    def remote(src, dst, send, recv, target):
        return pltpu.make_async_remote_copy(
            src_ref=src, dst_ref=dst, send_sem=send, recv_sem=recv,
            device_id={"ctx": target}, device_id_type=pl.DeviceIdType.MESH,
        )

    sends_far = device + reach < size
    gets_far = device >= reach
    crossing = (side == 1) & sends_far
    passes = (side == 0) & (device + 2 * reach < size)
    gets_passed = (side == 0) & gets_far
    partner = device + 1 - 2 * odd
    across = device ^ 2
    above = jnp.minimum(device + 4, last)
    below = jnp.maximum(device - 4, 0)
    has_above = line < length - 1
    has_below = line > 0

    barrier = pltpu.get_barrier_semaphore()
    greeted = (
        (has_above, above), (has_below, below),
        (crossing, device + reach), (gets_passed, device - reach),
    )

    def greet(target):
        pl.semaphore_signal(
            barrier, inc=1, device_id={"ctx": target}, device_id_type=pl.DeviceIdType.MESH
        )

    greet(partner)
    greet(across)
    arrivals = jnp.int32(2)
    for condition, target in greeted:
        @pl.when(condition)
        def _(target=target):
            greet(target)

        arrivals = arrivals + condition.astype(jnp.int32)

    rows_i = lax.broadcasted_iota(jnp.int32, (BLOCK, BLOCK), 0)
    cols_i = lax.broadcasted_iota(jnp.int32, (BLOCK, BLOCK), 1)
    diagonal[...] = jnp.where(cols_i >= rows_i, 0.0, MASKED).astype(jnp.bfloat16)
    unit[...] = jnp.where(rows_i == cols_i, 1.0, 0.0).astype(jnp.bfloat16)

    def own_block(block, carry):
        rows = pl.ds(pl.multiple_of(block * BLOCK, BLOCK), BLOCK)
        for kv, ref in enumerate((k_ref, v_ref)):
            for head in range(kv_heads):
                tile = ref[rows, head, :]
                own_ref[head, block, kv] = tile
                windows[head][reach * per_dev + block, kv] = tile
        return carry

    with jax.named_scope("own"):
        lax.fori_loop(0, per_dev, own_block, 0)

    def one_head(head, carry):
        for v in range(n_vert):
            at = vb_ref[v, head] - device * per_dev
            mine = (v < vc_ref[head]) & (at >= 0) & (at < per_dev)
            at = jnp.clip(at, 0, per_dev - 1)
            for kv in range(2):
                tile = own_ref[head, at, kv].astype(jnp.float32)
                row = pl.multiple_of(((head * n_vert + v) * 2 + kv) * BLOCK, BLOCK)
                acc[pl.ds(row, BLOCK), :] = jnp.where(mine, tile, 0.0).astype(jnp.bfloat16)
        return carry

    with jax.named_scope("terms"):
        lax.fori_loop(0, kv_heads, one_head, 0)
    with jax.named_scope("entry"):
        pl.semaphore_wait(barrier, arrivals)

    def place(head, where):
        return windows[head].at[pl.ds(where * per_dev, per_dev)]

    def far_copy(head):
        target = jnp.minimum(device + reach, last)
        return remote(own_ref.at[head], place(head, 0), far_send.at[head], far_recv.at[head], target)

    def stage_copy(head):
        slot = stage.at[head - direct]
        target = jnp.maximum(device - reach, 0)
        return remote(own_ref.at[head], slot, far_send.at[head], pass_recv.at[head - direct], target)

    def pass_copy(head):
        slot = stage.at[head - direct]
        return remote(
            slot, place(head, 0), pass_send.at[head - direct], far_recv.at[head], above
        )

    def near_copy(head):
        return remote(
            own_ref.at[head], place(head, 1), near_send.at[head], near_recv.at[head], partner
        )

    def relay_copy(head):
        return remote(
            place(head, 0), place(head, 1), near_send.at[head], near_recv.at[head], partner
        )

    def start_far(condition, heads):
        @pl.when(condition)
        def _():
            for head in heads:
                far_copy(head).start()

    def pass_on(heads):
        @pl.when(passes)
        def _():
            for head in heads:
                with jax.named_scope(f"stage#h={head}"):
                    stage_copy(head).wait_recv()
                pass_copy(head).start()

    chunk_rows = kv_heads * n_vert * 2 * BLOCK // CHUNKS
    half = chunk_rows // 2
    piece = half // length
    chunks = range(CHUNKS)

    def kept(c):
        return c * chunk_rows + odd * half

    def part(c, d):
        return pl.ds(pl.multiple_of(kept(c) + d * piece, 16), piece)

    def spot(c, d, way):
        return pl.ds(pl.multiple_of(((c * length + d) * 2 + way) * piece, 16), piece)

    def add(dst, at, landing, rows):
        step = min(rows, 256)

        def body(i, carry):
            here = pl.ds(pl.multiple_of(at + i * step, 16), step)
            there = pl.ds(pl.multiple_of(landing + i * step, 16), step)
            dst[here, :] = acc[here, :] + landed[there, :]
            return carry

        lax.fori_loop(0, rows // step, body, 0)

    def core_copy(c):
        given = pl.multiple_of(c * chunk_rows + (1 - odd) * half, 16)
        return remote(
            acc.at[pl.ds(given, half)], landed.at[pl.ds(landed_core + c * half, half)],
            core_send.at[c], core_recv.at[c], partner,
        )

    landed_core = CHUNKS * length * 2 * piece
    landed_swap = landed_core + CHUNKS * half

    def line_copy(c, d, way):
        recv = up_recv if way == 0 else down_recv
        target = above if way == 0 else below
        return remote(
            acc.at[part(c, d)], landed.at[spot(c, d, way)],
            line_send.at[c, d], recv.at[c, d], target,
        )

    def take(c, d, way):
        line_copy(c, d, way).wait_recv()
        add(acc, kept(c) + d * piece, ((c * length + d) * 2 + way) * piece, piece)

    def fold_line(c):
        for d in range(length - 1, 0, -1):
            @pl.when(line < d)
            def _(d=d):
                @pl.when(has_below)
                def _():
                    take(c, d, 0)

                line_copy(c, d, 0).start()

        for d in range(length - 1):
            @pl.when(line > d)
            def _(d=d):
                @pl.when(has_above)
                def _():
                    take(c, d, 1)

                line_copy(c, d, 1).start()

    def finish_line(c):
        @pl.when(has_below)
        def _():
            take(c, line, 0)

        @pl.when(has_above)
        def _():
            take(c, line, 1)

    def swap_copy(c):
        return remote(
            acc.at[part(c, line)], landed.at[pl.ds(landed_swap + c * piece, piece)],
            swap_send.at[c], swap_recv.at[c], across,
        )

    def spread_copy(c, d, way):
        send = above_send if way == 0 else below_send
        target = above if way == 0 else below
        return remote(
            full.at[part(c, d)], full.at[part(c, d)], send.at[c, d], spread_recv.at[c, d], target
        )

    def spread_own(c):
        swap_copy(c).wait_recv()
        add(full, kept(c) + line * piece, landed_swap + c * piece, piece)

        @pl.when(has_above)
        def _():
            spread_copy(c, line, 0).start()

        @pl.when(has_below)
        def _():
            spread_copy(c, line, 1).start()

    def spread_rest(c):
        for k in range(1, length):
            for way, d, found in ((0, line - k, line >= k), (1, line + k, line + k < length)):
                @pl.when(found)
                def _(way=way, d=d):
                    spread_copy(c, d, way).wait_recv()

                    @pl.when(has_above if way == 0 else has_below)
                    def _():
                        spread_copy(c, d, way).start()

    def grow_copy(c):
        rows = pl.ds(pl.multiple_of(kept(c), 16), half)
        return remote(full.at[rows], full.at[rows], grow_send.at[c], grow_recv.at[c], partner)

    early = 3 * kv_heads // 8
    for c in chunks:
        core_copy(c).start()
    start_far(side == 0, range(early))

    @pl.when(crossing)
    def _():
        for head in range(direct, kv_heads):
            stage_copy(head).start()

    @pl.when(odd == 0)
    def _():
        for head in range(kv_heads):
            near_copy(head).start()

    for c in chunks:
        with jax.named_scope(f"core#c={c}"):
            core_copy(c).wait_recv()
            add(acc, kept(c), landed_core + c * half, half)
        with jax.named_scope(f"fold#c={c}"):
            fold_line(c)

    def queries(block, carry):
        rows = pl.ds(pl.multiple_of(block * BLOCK, BLOCK), BLOCK)
        for h in range(kv_heads * group_size):
            qs_ref[rows, h * head_dim : (h + 1) * head_dim] = q_ref[rows, h, :]
        return carry

    start_far(crossing, range(min(2, direct)))
    for c in chunks:
        with jax.named_scope(f"finish#c={c}"):
            finish_line(c)
        swap_copy(c).start()
    start_far(side == 0, range(early, kv_heads))
    with jax.named_scope("queries#p=0"):
        lax.fori_loop(0, per_dev // 2, queries, 0)
    for c in chunks:
        with jax.named_scope(f"swap#c={c}"):
            spread_own(c)
    with jax.named_scope("queries#p=1"):
        lax.fori_loop(per_dev // 2, per_dev, queries, 0)
    for c in chunks:
        with jax.named_scope(f"spread#c={c}"):
            spread_rest(c)
        grow_copy(c).start()
    start_far(crossing, range(min(2, direct), direct))
    pass_on(range(direct, kv_heads))

    heads_chunk = kv_heads // CHUNKS
    for head in range(kv_heads):
        with jax.named_scope(f"far#h={head}"):
            @pl.when(gets_far)
            def _():
                far_copy(head).wait_recv()

                @pl.when(odd == 1)
                def _():
                    relay_copy(head).start()

        with jax.named_scope(f"near#h={head}"):
            @pl.when((odd == 1) | gets_far)
            def _():
                near_copy(head).wait_recv()

        if head % heads_chunk == 0:
            with jax.named_scope(f"grow#h={head}"):
                grow_copy(head // heads_chunk).wait_recv()
        with jax.named_scope(f"attend#h={head}"):
            attend_head(
                head, dims, device, tables, qs_ref, windows[head], full, diagonal, unit, out_ref
            )

    @pl.when(sends_far)
    def _():
        for head in range(kv_heads):
            far_copy(head).wait_send()

    @pl.when((odd == 0) | gets_far)
    def _():
        for head in range(kv_heads):
            near_copy(head).wait_send()

    @pl.when(passes)
    def _():
        for head in range(direct, kv_heads):
            pass_copy(head).wait_send()

    for c in chunks:
        core_copy(c).wait_send()
        swap_copy(c).wait_send()
        grow_copy(c).wait_send()
        for d in range(length):
            @pl.when(line != d)
            def _(d=d):
                line_copy(c, d, 0).wait_send()

            @pl.when((line >= d) & has_above)
            def _(d=d):
                spread_copy(c, d, 0).wait_send()

            @pl.when((line <= d) & has_below)
            def _(d=d):
                spread_copy(c, d, 1).wait_send()


def fused(keys, values, queries, vert_blocks, vert_count, slash_offsets, slash_count):
    size = lax.axis_size("ctx")
    rows_dev, kv_heads, head_dim = keys.shape
    q_heads = queries.shape[1]
    per_dev = rows_dev // BLOCK
    n_vert = vert_blocks.shape[0]
    n_slash = slash_offsets.shape[0]
    reach = -(-LARGEST_OFFSET // per_dev)
    relayed = 3 * kv_heads // 8
    length = size // 4
    dims = (per_dev, reach, n_vert, n_slash, q_heads // kv_heads, head_dim)
    dma = pltpu.SemaphoreType.DMA
    kind = keys.dtype
    column_rows = kv_heads * n_vert * 2 * BLOCK
    columns = pltpu.VMEM((column_rows, head_dim), kind)
    landed_rows = column_rows + column_rows // 2 + column_rows // 2 // length
    square = pltpu.VMEM((BLOCK, BLOCK), kind)
    window = pltpu.VMEM(((reach + 1) * per_dev, 2, BLOCK, head_dim), kind)
    smem = pl.BlockSpec(memory_space=pltpu.SMEM)
    vmem = pl.BlockSpec(memory_space=pltpu.VMEM)
    return pl.pallas_call(
        functools.partial(fused_kernel, size, kv_heads, relayed, dims),
        out_shape=jax.ShapeDtypeStruct((rows_dev, q_heads * head_dim), kind),
        in_specs=[smem] * 4 + [vmem] * 3,
        out_specs=vmem,
        scratch_shapes=[
            pltpu.VMEM((kv_heads, per_dev, 2, BLOCK, head_dim), kind),
            pltpu.VMEM((rows_dev, q_heads * head_dim), kind),
            columns,
            pltpu.VMEM((landed_rows, head_dim), kind),
            columns,
            pltpu.VMEM((relayed, per_dev, 2, BLOCK, head_dim), kind),
            square,
            square,
        ]
        + [window] * kv_heads
        + [dma((CHUNKS,))] * 6
        + [dma((CHUNKS, length))] * 6
        + [dma((kv_heads,))] * 4
        + [dma((relayed,))] * 2,
        compiler_params=pltpu.CompilerParams(
            collective_id=0, has_side_effects=True, vmem_limit_bytes=40 * 1024 * 1024
        ),
        name="fused",
    )(vert_blocks, vert_count, slash_offsets, slash_count, keys, values, queries)


def local(
    query_states, key_states, value_states, vert_blocks, vert_count, slash_offsets, slash_count
):
    out = fused(
        key_states,
        value_states,
        query_states,
        vert_blocks.T,
        vert_count,
        slash_offsets.T,
        slash_count,
    )
    return out.reshape(query_states.shape)


def solution(mesh):
    in_specs = (
        P(("groups", "ctx"), None, None),
        P(("groups", "ctx"), None, None),
        P(("groups", "ctx"), None, None),
        P("groups", None),
        P("groups"),
        P("groups", None),
        P("groups"),
    )
    out_specs = P(("groups", "ctx"), None, None)
    return jax.shard_map(local, mesh=mesh, in_specs=in_specs, out_specs=out_specs, check_vma=False)
```

```python
import functools
import math

import jax
import jax.numpy as jnp
from jax import lax
from jax.experimental import pallas as pl
from jax.experimental.pallas import tpu as pltpu
from jax.sharding import PartitionSpec as P

BLOCK = 128
LARGEST_OFFSET = 8
MASKED = -1e30
CHUNKS = 2


def attend_head(head, dims, device, tables, q_ref, window, columns, diagonal, unit, out_ref):
    per_dev, reach, n_vert, n_slash, group_size, head_dim = dims
    vb_ref, vc_ref, so_ref, sc_ref = tables
    scale = math.log2(math.e) / math.sqrt(head_dim)
    n_tiles = n_vert + n_slash
    chunk = 2 if group_size % 2 == 0 else 1
    parts = group_size // chunk

    def one_block(block, carry):
        qblock = device * per_dev + block
        start = pl.multiple_of(block * BLOCK, BLOCK)
        own = reach * per_dev + block
        spots, usable = [own], []
        for s in range(1, n_slash):
            offset = so_ref[s, head]
            ok = (s < sc_ref[head]) & (offset <= qblock)
            for v in range(n_vert):
                ok = ok & ((v >= vc_ref[head]) | (vb_ref[v, head] != qblock - offset))
            usable.append(ok)
            spots.append(jnp.where(ok, own - offset, own))
        for v in range(n_vert):
            usable.append((v < vc_ref[head]) & (vb_ref[v, head] < qblock))
        keys = [window[spot, 0] for spot in spots]
        values = [window[spot, 1] for spot in spots]
        for v in range(n_vert):
            row = (head * n_vert + v) * 2 * BLOCK
            keys.append(columns[row : row + BLOCK, :])
            values.append(columns[row + BLOCK : row + 2 * BLOCK, :])
        masks = [diagonal[...]]
        for ok in usable:
            fill = jnp.where(ok, 0.0, MASKED).astype(jnp.float32)
            masks.append(jnp.full((BLOCK, BLOCK), fill, jnp.float32).astype(jnp.bfloat16))
        keys = jnp.concatenate(
            [jnp.concatenate(keys, axis=0), jnp.concatenate(masks, axis=0)], axis=1
        )
        values = jnp.concatenate(values, axis=0)

        def scores_of(part):
            queries = []
            for h in range(part * chunk, (part + 1) * chunk):
                lane = (head * group_size + h) * head_dim
                rows = q_ref[pl.ds(start, BLOCK), lane : lane + head_dim]
                queries.append(jnp.concatenate([rows, unit[...]], axis=1))
            tile = lax.dot_general(
                jnp.concatenate(queries, axis=0), keys, (((1,), (1,)), ((), ())),
                preferred_element_type=jnp.float32,
            )
            return [tile[:, i * BLOCK : (i + 1) * BLOCK] for i in range(n_tiles)]

        def top_of(scores):
            return jnp.max(functools.reduce(jnp.maximum, scores), axis=1, keepdims=True)

        def sums_of(scores, top):
            powers = [jnp.exp2((tile - top) * scale) for tile in scores]
            total = jnp.sum(functools.reduce(jnp.add, powers), axis=1, keepdims=True)
            weights = jnp.concatenate([p.astype(jnp.bfloat16) for p in powers], axis=1)
            return jnp.dot(weights, values, preferred_element_type=jnp.float32), total

        def store(part, sums):
            result = (sums[0] / sums[1]).astype(jnp.bfloat16)
            for i in range(chunk):
                lane = (head * group_size + part * chunk + i) * head_dim
                out_ref[pl.ds(start, BLOCK), lane : lane + head_dim] = result[
                    i * BLOCK : (i + 1) * BLOCK
                ]

        scores = scores_of(0)
        top = top_of(scores)
        last = None
        for part in range(parts):
            following = scores_of(part + 1) if part + 1 < parts else None
            sums = sums_of(scores, top)
            if following is not None:
                top = top_of(following)
            if last is not None:
                store(part - 1, last)
            scores, last = following, sums
        store(parts - 1, last)
        return carry

    lax.fori_loop(0, per_dev, one_block, 0, unroll=2 if per_dev % 2 == 0 else 1)


def fused_kernel(
    size, kv_heads, relayed, dims,
    vb_hbm, vc_hbm, so_hbm, sc_hbm, k_hbm, v_hbm, q_hbm, out_hbm,
    vb_ref, vc_ref, so_ref, sc_ref, k_ref, v_ref, q_ref, out_ref, own_ref, qs_ref, acc, landed, full, stage, diagonal, unit, *scratch,
):
    per_dev, reach, n_vert, n_slash, group_size, head_dim = dims
    windows = scratch[:kv_heads]
    (
        load_sem, out_sem, core_send, core_recv, grow_send, grow_recv, swap_send, swap_recv,
        up_recv, down_recv, line_send, spread_recv, above_send, below_send,
        far_send, far_recv, near_send, near_recv, pass_send, pass_recv,
    ) = scratch[kv_heads:]
    tables = (vb_ref, vc_ref, so_ref, sc_ref)
    device = lax.axis_index("ctx")
    odd = lax.rem(device, 2)
    side = lax.rem(device // 2, 2)
    line = device // 4
    length = size // 4
    direct = kv_heads - relayed
    last = size - 1

    def remote(src, dst, send, recv, target):
        return pltpu.make_async_remote_copy(
            src_ref=src, dst_ref=dst, send_sem=send, recv_sem=recv,
            device_id={"ctx": target}, device_id_type=pl.DeviceIdType.MESH,
        )

    loads = [
        pltpu.make_async_copy(src, dst, load_sem.at[i])
        for i, (src, dst) in enumerate((
            (k_hbm, k_ref), (v_hbm, v_ref), (vb_hbm, vb_ref), (vc_hbm, vc_ref),
            (so_hbm, so_ref), (sc_hbm, sc_ref), (q_hbm, q_ref),
        ))
    ]
    for load in loads:
        load.start()

    sends_far = device + reach < size
    gets_far = device >= reach
    crossing = (side == 1) & sends_far
    passes = (side == 0) & (device + 2 * reach < size)
    gets_passed = (side == 0) & gets_far
    partner = device + 1 - 2 * odd
    across = device ^ 2
    above = jnp.minimum(device + 4, last)
    below = jnp.maximum(device - 4, 0)
    has_above = line < length - 1
    has_below = line > 0

    barrier = pltpu.get_barrier_semaphore()
    greeted = (
        (has_above, above), (has_below, below),
        (crossing, device + reach), (gets_passed, device - reach),
    )

    def greet(target):
        pl.semaphore_signal(
            barrier, inc=1, device_id={"ctx": target}, device_id_type=pl.DeviceIdType.MESH
        )

    greet(partner)
    greet(across)
    arrivals = jnp.int32(2)
    for condition, target in greeted:
        @pl.when(condition)
        def _(target=target):
            greet(target)

        arrivals = arrivals + condition.astype(jnp.int32)

    rows_i = lax.broadcasted_iota(jnp.int32, (BLOCK, BLOCK), 0)
    cols_i = lax.broadcasted_iota(jnp.int32, (BLOCK, BLOCK), 1)
    diagonal[...] = jnp.where(cols_i >= rows_i, 0.0, MASKED).astype(jnp.bfloat16)
    unit[...] = jnp.where(rows_i == cols_i, 1.0, 0.0).astype(jnp.bfloat16)

    def own_block(block, carry):
        rows = pl.ds(pl.multiple_of(block * BLOCK, BLOCK), BLOCK)
        for kv, ref in enumerate((k_ref, v_ref)):
            for head in range(kv_heads):
                tile = ref[rows, head, :]
                own_ref[head, block, kv] = tile
                windows[head][reach * per_dev + block, kv] = tile
        return carry

    with jax.named_scope("loads"):
        for load in loads[:-1]:
            load.wait()
    with jax.named_scope("own"):
        lax.fori_loop(0, per_dev, own_block, 0)

    def one_head(head, carry):
        for v in range(n_vert):
            at = vb_ref[v, head] - device * per_dev
            mine = (v < vc_ref[head]) & (at >= 0) & (at < per_dev)
            at = jnp.clip(at, 0, per_dev - 1)
            for kv in range(2):
                tile = own_ref[head, at, kv].astype(jnp.float32)
                row = pl.multiple_of(((head * n_vert + v) * 2 + kv) * BLOCK, BLOCK)
                acc[pl.ds(row, BLOCK), :] = jnp.where(mine, tile, 0.0).astype(jnp.bfloat16)
        return carry

    with jax.named_scope("terms"):
        lax.fori_loop(0, kv_heads, one_head, 0)
    with jax.named_scope("entry"):
        pl.semaphore_wait(barrier, arrivals)

    def place(head, where):
        return windows[head].at[pl.ds(where * per_dev, per_dev)]

    def far_copy(head):
        target = jnp.minimum(device + reach, last)
        return remote(own_ref.at[head], place(head, 0), far_send.at[head], far_recv.at[head], target)

    def stage_copy(head):
        slot = stage.at[head - direct]
        target = jnp.maximum(device - reach, 0)
        return remote(own_ref.at[head], slot, far_send.at[head], pass_recv.at[head - direct], target)

    def pass_copy(head):
        slot = stage.at[head - direct]
        return remote(
            slot, place(head, 0), pass_send.at[head - direct], far_recv.at[head], above
        )

    def near_copy(head):
        return remote(
            own_ref.at[head], place(head, 1), near_send.at[head], near_recv.at[head], partner
        )

    def relay_copy(head):
        return remote(
            place(head, 0), place(head, 1), near_send.at[head], near_recv.at[head], partner
        )

    def start_far(condition, heads):
        @pl.when(condition)
        def _():
            for head in heads:
                far_copy(head).start()

    def pass_on(condition, heads):
        @pl.when(passes & condition)
        def _():
            for head in heads:
                with jax.named_scope(f"stage#h={head}"):
                    stage_copy(head).wait_recv()
                pass_copy(head).start()

    chunk_rows = kv_heads * n_vert * 2 * BLOCK // CHUNKS
    half = chunk_rows // 2
    piece = half // length
    chunks = range(CHUNKS)

    def kept(c):
        return c * chunk_rows + odd * half

    def part(c, d):
        return pl.ds(pl.multiple_of(kept(c) + d * piece, 16), piece)

    def spot(c, d, way):
        return pl.ds(pl.multiple_of(((c * length + d) * 2 + way) * piece, 16), piece)

    def add(dst, at, landing, rows):
        step = min(rows, 256)

        def body(i, carry):
            here = pl.ds(pl.multiple_of(at + i * step, 16), step)
            there = pl.ds(pl.multiple_of(landing + i * step, 16), step)
            dst[here, :] = acc[here, :] + landed[there, :]
            return carry

        lax.fori_loop(0, rows // step, body, 0)

    def core_copy(c):
        given = pl.multiple_of(c * chunk_rows + (1 - odd) * half, 16)
        return remote(
            acc.at[pl.ds(given, half)], landed.at[pl.ds(landed_core + c * half, half)],
            core_send.at[c], core_recv.at[c], partner,
        )

    landed_core = CHUNKS * length * 2 * piece
    landed_swap = landed_core + CHUNKS * half

    def line_copy(c, d, way):
        recv = up_recv if way == 0 else down_recv
        target = above if way == 0 else below
        return remote(
            acc.at[part(c, d)], landed.at[spot(c, d, way)],
            line_send.at[c, d], recv.at[c, d], target,
        )

    def take(c, d, way):
        line_copy(c, d, way).wait_recv()
        add(acc, kept(c) + d * piece, ((c * length + d) * 2 + way) * piece, piece)

    def fold_up(c):
        for d in range(length - 1, 0, -1):
            @pl.when(line < d)
            def _(d=d):
                @pl.when(has_below)
                def _():
                    take(c, d, 0)

                line_copy(c, d, 0).start()

    def fold_down(c):
        for d in range(length - 1):
            @pl.when(line > d)
            def _(d=d):
                @pl.when(has_above)
                def _():
                    take(c, d, 1)

                line_copy(c, d, 1).start()

    lower = 2 * line < length

    def fold_line(c):
        @pl.when(lower)
        def _():
            fold_up(c)
            fold_down(c)

        @pl.when(jnp.logical_not(lower))
        def _():
            fold_down(c)
            fold_up(c)

    def finish_line(c):
        @pl.when(has_below)
        def _():
            take(c, line, 0)

        @pl.when(has_above)
        def _():
            take(c, line, 1)

    def swap_copy(c):
        return remote(
            acc.at[part(c, line)], landed.at[pl.ds(landed_swap + c * piece, piece)],
            swap_send.at[c], swap_recv.at[c], across,
        )

    def spread_copy(c, d, way):
        send = above_send if way == 0 else below_send
        target = above if way == 0 else below
        return remote(
            full.at[part(c, d)], full.at[part(c, d)], send.at[c, d], spread_recv.at[c, d], target
        )

    def spread_own(c):
        swap_copy(c).wait_recv()
        add(full, kept(c) + line * piece, landed_swap + c * piece, piece)

        @pl.when(has_above)
        def _():
            spread_copy(c, line, 0).start()

        @pl.when(has_below)
        def _():
            spread_copy(c, line, 1).start()

    def spread_rest(c):
        for k in range(1, length):
            for way, d, found in ((0, line - k, line >= k), (1, line + k, line + k < length)):
                @pl.when(found)
                def _(way=way, d=d):
                    spread_copy(c, d, way).wait_recv()

                    @pl.when(has_above if way == 0 else has_below)
                    def _():
                        spread_copy(c, d, way).start()

    def grow_copy(c):
        rows = pl.ds(pl.multiple_of(kept(c), 16), half)
        return remote(full.at[rows], full.at[rows], grow_send.at[c], grow_recv.at[c], partner)

    early = kv_heads // 4
    middle = has_above & has_below
    edge = jnp.logical_not(middle)

    def stage_on(heads):
        @pl.when(crossing)
        def _():
            for head in heads:
                stage_copy(head).start()

    for c in chunks:
        core_copy(c).start()
    start_far(side == 0, range(early))
    stage_on(range(direct, direct + 2))
    start_far(crossing & (line == length - 2) & (line > 0), range(2))

    @pl.when(odd == 0)
    def _():
        for head in range(kv_heads):
            near_copy(head).start()

    for c in chunks:
        with jax.named_scope(f"core#c={c}"):
            core_copy(c).wait_recv()
            add(acc, kept(c), landed_core + c * half, half)
        if c == 0:
            with jax.named_scope(f"fold#c={c}"):
                fold_line(c)

    def queries(block, carry):
        rows = pl.ds(pl.multiple_of(block * BLOCK, BLOCK), BLOCK)
        for h in range(kv_heads * group_size):
            qs_ref[rows, h * head_dim : (h + 1) * head_dim] = q_ref[rows, h, :]
        return carry

    @pl.when(edge)
    def _():
        with jax.named_scope("fold_edge#c=1"):
            fold_line(1)

    with jax.named_scope("finish#c=0"):
        finish_line(0)
    swap_copy(0).start()
    stage_on(range(direct + 2, direct + 3))
    pass_on((line == length - 2) & (line > 0), range(direct, direct + 2))

    @pl.when(middle)
    def _():
        with jax.named_scope("fold_mid#c=1"):
            fold_line(1)

    loads[-1].wait()
    with jax.named_scope("queries#p=0"):
        lax.fori_loop(0, per_dev // 2, queries, 0)
    with jax.named_scope("swap#c=0"):
        spread_own(0)
    with jax.named_scope("finish#c=1"):
        finish_line(1)
    swap_copy(1).start()
    start_far(side == 0, range(early, kv_heads))
    stage_on(range(direct + 3, kv_heads))
    with jax.named_scope("queries#p=1"):
        lax.fori_loop(per_dev // 2, per_dev, queries, 0)
    with jax.named_scope("swap#c=1"):
        spread_own(1)
    late = (line != length - 2) | (line == 0)
    start_far(crossing & (line == 0), range(2))
    pass_on(line == 0, range(direct, direct + 2))
    with jax.named_scope("spread#c=0"):
        spread_rest(0)
    grow_copy(0).start()
    start_far(crossing & late & (line > 0), range(1))
    pass_on(late & (line > 0), range(direct, direct + 1))

    heads_chunk = kv_heads // CHUNKS

    def get_head(head):
        with jax.named_scope(f"far#h={head}"):
            @pl.when(gets_far)
            def _():
                far_copy(head).wait_recv()

                @pl.when(odd == 1)
                def _():
                    relay_copy(head).start()

        with jax.named_scope(f"near#h={head}"):
            @pl.when((odd == 1) | gets_far)
            def _():
                near_copy(head).wait_recv()

    def out_copy(head):
        lanes = pl.ds(head * group_size * head_dim, group_size * head_dim)
        return pltpu.make_async_copy(out_ref.at[:, lanes], out_hbm.at[:, lanes], out_sem.at[head])

    def do_head(head):
        with jax.named_scope(f"attend#h={head}"):
            attend_head(
                head, dims, device, tables, qs_ref, windows[head], full, diagonal, unit, out_ref
            )
        out_copy(head).start()

    with jax.named_scope("spread#c=1"):
        spread_rest(1)
    grow_copy(1).start()
    start_far(crossing & late & (line > 0), range(1, 2))
    pass_on(late & (line > 0), range(direct + 1, direct + 2))
    start_far(crossing, range(2, direct))
    with jax.named_scope("grow#c=0"):
        grow_copy(0).wait_recv()

    order = [h for i in range(kv_heads) for h in (i, direct + i) if i < direct and h < kv_heads]
    for head in order:
        get_head(head)
        if head == next(h for h in order if h >= heads_chunk):
            with jax.named_scope("grow#c=1"):
                grow_copy(1).wait_recv()
        do_head(head)
        step = order.index(head)
        if step >= 1 and direct + 1 + step < kv_heads:
            pass_on(line >= 0, range(direct + 1 + step, direct + 2 + step))

    for head in range(kv_heads):
        out_copy(head).wait()

    @pl.when(sends_far)
    def _():
        for head in range(kv_heads):
            far_copy(head).wait_send()

    @pl.when((odd == 0) | gets_far)
    def _():
        for head in range(kv_heads):
            near_copy(head).wait_send()

    @pl.when(passes)
    def _():
        for head in range(direct, kv_heads):
            pass_copy(head).wait_send()

    for c in chunks:
        core_copy(c).wait_send()
        swap_copy(c).wait_send()
        grow_copy(c).wait_send()
        for d in range(length):
            @pl.when(line != d)
            def _(d=d):
                line_copy(c, d, 0).wait_send()

            @pl.when((line >= d) & has_above)
            def _(d=d):
                spread_copy(c, d, 0).wait_send()

            @pl.when((line <= d) & has_below)
            def _(d=d):
                spread_copy(c, d, 1).wait_send()


def fused(keys, values, queries, vert_blocks, vert_count, slash_offsets, slash_count):
    size = lax.axis_size("ctx")
    rows_dev, kv_heads, head_dim = keys.shape
    q_heads = queries.shape[1]
    per_dev = rows_dev // BLOCK
    n_vert = vert_blocks.shape[0]
    n_slash = slash_offsets.shape[0]
    reach = -(-LARGEST_OFFSET // per_dev)
    relayed = kv_heads // 2
    length = size // 4
    dims = (per_dev, reach, n_vert, n_slash, q_heads // kv_heads, head_dim)
    dma = pltpu.SemaphoreType.DMA
    kind = keys.dtype
    column_rows = kv_heads * n_vert * 2 * BLOCK
    columns = pltpu.VMEM((column_rows, head_dim), kind)
    landed_rows = column_rows + column_rows // 2 + column_rows // 2 // length
    square = pltpu.VMEM((BLOCK, BLOCK), kind)
    window = pltpu.VMEM(((reach + 1) * per_dev, 2, BLOCK, head_dim), kind)
    hbm = pl.BlockSpec(memory_space=pltpu.HBM)
    return pl.pallas_call(
        functools.partial(fused_kernel, size, kv_heads, relayed, dims),
        out_shape=jax.ShapeDtypeStruct((rows_dev, q_heads * head_dim), kind),
        in_specs=[hbm] * 7,
        out_specs=hbm,
        scratch_shapes=[
            pltpu.SMEM(vert_blocks.shape, jnp.int32),
            pltpu.SMEM(vert_count.shape, jnp.int32),
            pltpu.SMEM(slash_offsets.shape, jnp.int32),
            pltpu.SMEM(slash_count.shape, jnp.int32),
            pltpu.VMEM(keys.shape, kind),
            pltpu.VMEM(values.shape, kind),
            pltpu.VMEM(queries.shape, kind),
            pltpu.VMEM((rows_dev, q_heads * head_dim), kind),
            pltpu.VMEM((kv_heads, per_dev, 2, BLOCK, head_dim), kind),
            pltpu.VMEM((rows_dev, q_heads * head_dim), kind),
            columns,
            pltpu.VMEM((landed_rows, head_dim), kind),
            columns,
            pltpu.VMEM((relayed, per_dev, 2, BLOCK, head_dim), kind),
            square,
            square,
        ]
        + [window] * kv_heads
        + [dma((7,)), dma((kv_heads,))]
        + [dma((CHUNKS,))] * 6
        + [dma((CHUNKS, length))] * 6
        + [dma((kv_heads,))] * 4
        + [dma((relayed,))] * 2,
        compiler_params=pltpu.CompilerParams(
            collective_id=0, has_side_effects=True, vmem_limit_bytes=56 * 1024 * 1024
        ),
        name="fused",
    )(vert_blocks, vert_count, slash_offsets, slash_count, keys, values, queries)


def local(
    query_states, key_states, value_states, vert_blocks, vert_count, slash_offsets, slash_count
):
    out = fused(
        key_states,
        value_states,
        query_states,
        vert_blocks.T,
        vert_count,
        slash_offsets.T,
        slash_count,
    )
    return out.reshape(query_states.shape)


def solution(mesh):
    in_specs = (
        P(("groups", "ctx"), None, None),
        P(("groups", "ctx"), None, None),
        P(("groups", "ctx"), None, None),
        P("groups", None),
        P("groups"),
        P("groups", None),
        P("groups"),
    )
    out_specs = P(("groups", "ctx"), None, None)
    return jax.shard_map(local, mesh=mesh, in_specs=in_specs, out_specs=out_specs, check_vma=False)
```

```python
import functools
import math

import jax
import jax.numpy as jnp
from jax import lax
from jax.experimental import pallas as pl
from jax.experimental.pallas import tpu as pltpu
from jax.sharding import PartitionSpec as P

BLOCK = 128
LARGEST_OFFSET = 8
MASKED = -1e30
CHUNKS = 2


def attend_head(head, dims, device, tables, q_ref, window, columns, diagonal, unit, out_ref):
    per_dev, reach, n_vert, n_slash, group_size, head_dim = dims
    vb_ref, vc_ref, so_ref, sc_ref = tables
    scale = math.log2(math.e) / math.sqrt(head_dim)
    n_tiles = n_vert + n_slash
    chunk = 2 if group_size % 2 == 0 else 1
    parts = group_size // chunk

    def one_block(block, carry):
        qblock = device * per_dev + block
        start = pl.multiple_of(block * BLOCK, BLOCK)
        own = reach * per_dev + block
        spots, usable = [own], []
        for s in range(1, n_slash):
            offset = so_ref[s, head]
            ok = (s < sc_ref[head]) & (offset <= qblock)
            for v in range(n_vert):
                ok = ok & ((v >= vc_ref[head]) | (vb_ref[v, head] != qblock - offset))
            usable.append(ok)
            spots.append(jnp.where(ok, own - offset, own))
        for v in range(n_vert):
            usable.append((v < vc_ref[head]) & (vb_ref[v, head] < qblock))
        keys = [window[spot, 0] for spot in spots]
        values = [window[spot, 1] for spot in spots]
        for v in range(n_vert):
            row = (head * n_vert + v) * 2 * BLOCK
            keys.append(columns[row : row + BLOCK, :])
            values.append(columns[row + BLOCK : row + 2 * BLOCK, :])
        masks = [diagonal[...]]
        for ok in usable:
            fill = jnp.where(ok, 0.0, MASKED).astype(jnp.float32)
            masks.append(jnp.full((BLOCK, BLOCK), fill, jnp.float32).astype(jnp.bfloat16))
        keys = jnp.concatenate(
            [jnp.concatenate(keys, axis=0), jnp.concatenate(masks, axis=0)], axis=1
        )
        values = jnp.concatenate(values, axis=0)

        def scores_of(part):
            queries = []
            for h in range(part * chunk, (part + 1) * chunk):
                lane = (head * group_size + h) * head_dim
                rows = q_ref[pl.ds(start, BLOCK), lane : lane + head_dim]
                queries.append(jnp.concatenate([rows, unit[...]], axis=1))
            tile = lax.dot_general(
                jnp.concatenate(queries, axis=0), keys, (((1,), (1,)), ((), ())),
                preferred_element_type=jnp.float32,
            )
            return [tile[:, i * BLOCK : (i + 1) * BLOCK] for i in range(n_tiles)]

        def top_of(scores):
            return jnp.max(functools.reduce(jnp.maximum, scores), axis=1, keepdims=True)

        def sums_of(scores, top):
            powers = [jnp.exp2((tile - top) * scale) for tile in scores]
            total = jnp.sum(functools.reduce(jnp.add, powers), axis=1, keepdims=True)
            weights = jnp.concatenate([p.astype(jnp.bfloat16) for p in powers], axis=1)
            return jnp.dot(weights, values, preferred_element_type=jnp.float32), total

        def store(part, sums):
            result = (sums[0] / sums[1]).astype(jnp.bfloat16)
            for i in range(chunk):
                lane = (head * group_size + part * chunk + i) * head_dim
                out_ref[pl.ds(start, BLOCK), lane : lane + head_dim] = result[
                    i * BLOCK : (i + 1) * BLOCK
                ]

        scores = scores_of(0)
        top = top_of(scores)
        last = None
        for part in range(parts):
            following = scores_of(part + 1) if part + 1 < parts else None
            sums = sums_of(scores, top)
            if following is not None:
                top = top_of(following)
            if last is not None:
                store(part - 1, last)
            scores, last = following, sums
        store(parts - 1, last)
        return carry

    lax.fori_loop(0, per_dev, one_block, 0, unroll=2 if per_dev % 2 == 0 else 1)


def fused_kernel(
    size, kv_heads, relayed, dims,
    vb_hbm, vc_hbm, so_hbm, sc_hbm, k_hbm, v_hbm, q_hbm, out_hbm,
    vb_ref, vc_ref, so_ref, sc_ref, k_ref, v_ref, q_ref, out_ref, own_ref, qs_ref, acc, landed, full, stage, diagonal, unit, *scratch,
):
    per_dev, reach, n_vert, n_slash, group_size, head_dim = dims
    windows = scratch[:kv_heads]
    (
        load_sem, out_sem, core_send, core_recv, grow_send, grow_recv, swap_send, swap_recv,
        up_recv, down_recv, line_send, spread_recv, above_send, below_send,
        far_send, far_recv, near_send, near_recv, pass_send, pass_recv,
    ) = scratch[kv_heads:]
    tables = (vb_ref, vc_ref, so_ref, sc_ref)
    device = lax.axis_index("ctx")
    odd = lax.rem(device, 2)
    side = lax.rem(device // 2, 2)
    line = device // 4
    length = size // 4
    direct = kv_heads - relayed
    last = size - 1

    def remote(src, dst, send, recv, target):
        return pltpu.make_async_remote_copy(
            src_ref=src, dst_ref=dst, send_sem=send, recv_sem=recv,
            device_id={"ctx": target}, device_id_type=pl.DeviceIdType.MESH,
        )

    loads = [
        pltpu.make_async_copy(src, dst, load_sem.at[i])
        for i, (src, dst) in enumerate((
            (k_hbm, k_ref), (v_hbm, v_ref), (vb_hbm, vb_ref), (vc_hbm, vc_ref),
            (so_hbm, so_ref), (sc_hbm, sc_ref), (q_hbm, q_ref),
        ))
    ]
    for load in loads:
        load.start()

    sends_far = device + reach < size
    gets_far = device >= reach
    crossing = (side == 1) & sends_far
    passes = (side == 0) & (device + 2 * reach < size)
    gets_passed = (side == 0) & gets_far
    partner = device + 1 - 2 * odd
    across = device ^ 2
    above = jnp.minimum(device + 4, last)
    below = jnp.maximum(device - 4, 0)
    has_above = line < length - 1
    has_below = line > 0

    barrier = pltpu.get_barrier_semaphore()
    greeted = (
        (has_above, above), (has_below, below),
        (crossing, device + reach), (gets_passed, device - reach),
    )

    def greet(target):
        pl.semaphore_signal(
            barrier, inc=1, device_id={"ctx": target}, device_id_type=pl.DeviceIdType.MESH
        )

    greet(partner)
    greet(across)
    arrivals = jnp.int32(2)
    for condition, target in greeted:
        @pl.when(condition)
        def _(target=target):
            greet(target)

        arrivals = arrivals + condition.astype(jnp.int32)

    rows_i = lax.broadcasted_iota(jnp.int32, (BLOCK, BLOCK), 0)
    cols_i = lax.broadcasted_iota(jnp.int32, (BLOCK, BLOCK), 1)
    diagonal[...] = jnp.where(cols_i >= rows_i, 0.0, MASKED).astype(jnp.bfloat16)
    unit[...] = jnp.where(rows_i == cols_i, 1.0, 0.0).astype(jnp.bfloat16)

    def own_block(block, carry):
        rows = pl.ds(pl.multiple_of(block * BLOCK, BLOCK), BLOCK)
        for kv, ref in enumerate((k_ref, v_ref)):
            for head in range(kv_heads):
                tile = ref[rows, head, :]
                own_ref[head, block, kv] = tile
                windows[head][reach * per_dev + block, kv] = tile
        return carry

    with jax.named_scope("loads"):
        for load in loads[:-1]:
            load.wait()
    with jax.named_scope("own"):
        lax.fori_loop(0, per_dev, own_block, 0)

    def one_head(head, carry):
        for v in range(n_vert):
            at = vb_ref[v, head] - device * per_dev
            mine = (v < vc_ref[head]) & (at >= 0) & (at < per_dev)
            at = jnp.clip(at, 0, per_dev - 1)
            for kv in range(2):
                tile = own_ref[head, at, kv].astype(jnp.float32)
                row = pl.multiple_of(((head * n_vert + v) * 2 + kv) * BLOCK, BLOCK)
                acc[pl.ds(row, BLOCK), :] = jnp.where(mine, tile, 0.0).astype(jnp.bfloat16)
        return carry

    with jax.named_scope("terms"):
        lax.fori_loop(0, kv_heads, one_head, 0)
    with jax.named_scope("entry"):
        pl.semaphore_wait(barrier, arrivals)

    def place(head, where):
        return windows[head].at[pl.ds(where * per_dev, per_dev)]

    def far_copy(head):
        target = jnp.minimum(device + reach, last)
        return remote(own_ref.at[head], place(head, 0), far_send.at[head], far_recv.at[head], target)

    def stage_copy(head):
        slot = stage.at[head - direct]
        target = jnp.maximum(device - reach, 0)
        return remote(own_ref.at[head], slot, far_send.at[head], pass_recv.at[head - direct], target)

    def pass_copy(head):
        slot = stage.at[head - direct]
        return remote(
            slot, place(head, 0), pass_send.at[head - direct], far_recv.at[head], above
        )

    def near_copy(head):
        return remote(
            own_ref.at[head], place(head, 1), near_send.at[head], near_recv.at[head], partner
        )

    def relay_copy(head):
        return remote(
            place(head, 0), place(head, 1), near_send.at[head], near_recv.at[head], partner
        )

    def start_far(condition, heads):
        @pl.when(condition)
        def _():
            for head in heads:
                far_copy(head).start()

    def pass_on(condition, heads):
        @pl.when(passes & condition)
        def _():
            for head in heads:
                with jax.named_scope(f"stage#h={head}"):
                    stage_copy(head).wait_recv()
                pass_copy(head).start()

    chunk_rows = kv_heads * n_vert * 2 * BLOCK // CHUNKS
    half = chunk_rows // 2
    piece = half // length
    chunks = range(CHUNKS)

    def kept(c):
        return c * chunk_rows + odd * half

    def part(c, d):
        return pl.ds(pl.multiple_of(kept(c) + d * piece, 16), piece)

    def spot(c, d, way):
        return pl.ds(pl.multiple_of(((c * length + d) * 2 + way) * piece, 16), piece)

    def add(dst, at, landing, rows):
        step = min(rows, 256)

        def body(i, carry):
            here = pl.ds(pl.multiple_of(at + i * step, 16), step)
            there = pl.ds(pl.multiple_of(landing + i * step, 16), step)
            dst[here, :] = acc[here, :] + landed[there, :]
            return carry

        lax.fori_loop(0, rows // step, body, 0)

    def core_copy(c):
        given = pl.multiple_of(c * chunk_rows + (1 - odd) * half, 16)
        return remote(
            acc.at[pl.ds(given, half)], landed.at[pl.ds(landed_core + c * half, half)],
            core_send.at[c], core_recv.at[c], partner,
        )

    landed_core = CHUNKS * length * 2 * piece
    landed_swap = landed_core + CHUNKS * half

    def line_copy(c, d, way):
        recv = up_recv if way == 0 else down_recv
        target = above if way == 0 else below
        return remote(
            acc.at[part(c, d)], landed.at[spot(c, d, way)],
            line_send.at[c, d], recv.at[c, d], target,
        )

    def take(c, d, way):
        line_copy(c, d, way).wait_recv()
        add(acc, kept(c) + d * piece, ((c * length + d) * 2 + way) * piece, piece)

    def fold_up(c):
        for d in range(length - 1, 0, -1):
            @pl.when(line < d)
            def _(d=d):
                @pl.when(has_below)
                def _():
                    take(c, d, 0)

                line_copy(c, d, 0).start()

    def fold_down(c):
        for d in range(length - 1):
            @pl.when(line > d)
            def _(d=d):
                @pl.when(has_above)
                def _():
                    take(c, d, 1)

                line_copy(c, d, 1).start()

    lower = 2 * line < length

    def fold_line(c):
        @pl.when(lower)
        def _():
            fold_up(c)
            fold_down(c)

        @pl.when(jnp.logical_not(lower))
        def _():
            fold_down(c)
            fold_up(c)

    def finish_line(c):
        @pl.when(has_below)
        def _():
            take(c, line, 0)

        @pl.when(has_above)
        def _():
            take(c, line, 1)

    def swap_copy(c):
        return remote(
            acc.at[part(c, line)], landed.at[pl.ds(landed_swap + c * piece, piece)],
            swap_send.at[c], swap_recv.at[c], across,
        )

    def spread_copy(c, d, way):
        send = above_send if way == 0 else below_send
        target = above if way == 0 else below
        return remote(
            full.at[part(c, d)], full.at[part(c, d)], send.at[c, d], spread_recv.at[c, d], target
        )

    def spread_own(c):
        swap_copy(c).wait_recv()
        add(full, kept(c) + line * piece, landed_swap + c * piece, piece)

        @pl.when(has_above)
        def _():
            spread_copy(c, line, 0).start()

        @pl.when(has_below)
        def _():
            spread_copy(c, line, 1).start()

    def spread_rest(c):
        for k in range(1, length):
            for way, d, found in ((0, line - k, line >= k), (1, line + k, line + k < length)):
                @pl.when(found)
                def _(way=way, d=d):
                    spread_copy(c, d, way).wait_recv()

                    @pl.when(has_above if way == 0 else has_below)
                    def _():
                        spread_copy(c, d, way).start()

    def grow_copy(c):
        rows = pl.ds(pl.multiple_of(kept(c), 16), half)
        return remote(full.at[rows], full.at[rows], grow_send.at[c], grow_recv.at[c], partner)

    early = kv_heads // 4
    middle = has_above & has_below
    edge = jnp.logical_not(middle)

    def stage_on(heads):
        @pl.when(crossing)
        def _():
            for head in heads:
                stage_copy(head).start()

    for c in chunks:
        core_copy(c).start()
    start_far(side == 0, range(early))
    stage_on(range(direct, direct + 2))
    start_far(crossing & (line == length - 2) & (line > 0), range(2))

    @pl.when(odd == 0)
    def _():
        for head in range(kv_heads):
            near_copy(head).start()

    for c in chunks:
        with jax.named_scope(f"core#c={c}"):
            core_copy(c).wait_recv()
            add(acc, kept(c), landed_core + c * half, half)
        if c == 0:
            with jax.named_scope(f"fold#c={c}"):
                fold_line(c)

    def queries(block, carry):
        rows = pl.ds(pl.multiple_of(block * BLOCK, BLOCK), BLOCK)
        for h in range(kv_heads * group_size):
            qs_ref[rows, h * head_dim : (h + 1) * head_dim] = q_ref[rows, h, :]
        return carry

    @pl.when(edge)
    def _():
        with jax.named_scope("fold_edge#c=1"):
            fold_line(1)

    loads[-1].wait()

    @pl.when(edge)
    def _():
        with jax.named_scope("queries_edge"):
            lax.fori_loop(0, per_dev, queries, 0)

    with jax.named_scope("finish#c=0"):
        finish_line(0)
    swap_copy(0).start()
    stage_on(range(direct + 2, direct + 3))
    pass_on((line == length - 2) & (line > 0), range(direct, direct + 2))

    @pl.when(middle)
    def _():
        with jax.named_scope("fold_mid#c=1"):
            fold_line(1)

    with jax.named_scope("swap#c=0"):
        spread_own(0)
    with jax.named_scope("finish#c=1"):
        finish_line(1)
    swap_copy(1).start()
    start_far(side == 0, range(early, kv_heads))
    stage_on(range(direct + 3, kv_heads))

    @pl.when(middle)
    def _():
        with jax.named_scope("queries#p=0"):
            lax.fori_loop(0, per_dev // 2, queries, 0)

    with jax.named_scope("swap#c=1"):
        spread_own(1)
    late = (line != length - 2) | (line == 0)
    start_far(crossing & (line == 0), range(2))
    pass_on(line == 0, range(direct, direct + 2))
    with jax.named_scope("spread#c=0"):
        spread_rest(0)
    grow_copy(0).start()
    start_far(crossing & late & (line > 0), range(1))
    pass_on(late & (line > 0), range(direct, direct + 1))

    @pl.when(middle)
    def _():
        with jax.named_scope("queries#p=1"):
            lax.fori_loop(per_dev // 2, per_dev, queries, 0)


    heads_chunk = kv_heads // CHUNKS

    def get_head(head):
        with jax.named_scope(f"far#h={head}"):
            @pl.when(gets_far)
            def _():
                far_copy(head).wait_recv()

                @pl.when(odd == 1)
                def _():
                    relay_copy(head).start()

        with jax.named_scope(f"near#h={head}"):
            @pl.when((odd == 1) | gets_far)
            def _():
                near_copy(head).wait_recv()

    def out_copy(head):
        lanes = pl.ds(head * group_size * head_dim, group_size * head_dim)
        return pltpu.make_async_copy(out_ref.at[:, lanes], out_hbm.at[:, lanes], out_sem.at[head])

    def do_head(head):
        with jax.named_scope(f"attend#h={head}"):
            attend_head(
                head, dims, device, tables, qs_ref, windows[head], full, diagonal, unit, out_ref
            )
        out_copy(head).start()

    def do_first(heads):
        with jax.named_scope("grow#c=0"):
            grow_copy(0).wait_recv()
        for head in heads:
            get_head(head)
            do_head(head)

    @pl.when(edge)
    def _():
        do_first(range(2))

    with jax.named_scope("spread#c=1"):
        spread_rest(1)
    grow_copy(1).start()
    start_far(crossing & late & (line > 0), range(1, 2))
    pass_on(late & (line > 0), range(direct + 1, direct + 2))
    start_far(crossing, range(2, direct))

    @pl.when(middle)
    def _():
        do_first(range(1))

    with jax.named_scope("grow#c=1"):
        grow_copy(1).wait_recv()
    order = [h for i in range(kv_heads) for h in (i, direct + i) if i < direct and h < kv_heads]
    order = [h for h in order if h > 1]
    for step, head in enumerate(order):
        get_head(head)
        do_head(head)
        if step == 0:
            @pl.when(middle)
            def _():
                get_head(1)
                do_head(1)

        if direct + 2 + step < kv_heads:
            pass_on(line >= 0, range(direct + 2 + step, direct + 3 + step))

    for head in range(kv_heads):
        out_copy(head).wait()

    @pl.when(sends_far)
    def _():
        for head in range(kv_heads):
            far_copy(head).wait_send()

    @pl.when((odd == 0) | gets_far)
    def _():
        for head in range(kv_heads):
            near_copy(head).wait_send()

    @pl.when(passes)
    def _():
        for head in range(direct, kv_heads):
            pass_copy(head).wait_send()

    for c in chunks:
        core_copy(c).wait_send()
        swap_copy(c).wait_send()
        grow_copy(c).wait_send()
        for d in range(length):
            @pl.when(line != d)
            def _(d=d):
                line_copy(c, d, 0).wait_send()

            @pl.when((line >= d) & has_above)
            def _(d=d):
                spread_copy(c, d, 0).wait_send()

            @pl.when((line <= d) & has_below)
            def _(d=d):
                spread_copy(c, d, 1).wait_send()


def fused(keys, values, queries, vert_blocks, vert_count, slash_offsets, slash_count):
    size = lax.axis_size("ctx")
    rows_dev, kv_heads, head_dim = keys.shape
    q_heads = queries.shape[1]
    per_dev = rows_dev // BLOCK
    n_vert = vert_blocks.shape[0]
    n_slash = slash_offsets.shape[0]
    reach = -(-LARGEST_OFFSET // per_dev)
    relayed = kv_heads // 2
    length = size // 4
    dims = (per_dev, reach, n_vert, n_slash, q_heads // kv_heads, head_dim)
    dma = pltpu.SemaphoreType.DMA
    kind = keys.dtype
    column_rows = kv_heads * n_vert * 2 * BLOCK
    columns = pltpu.VMEM((column_rows, head_dim), kind)
    landed_rows = column_rows + column_rows // 2 + column_rows // 2 // length
    square = pltpu.VMEM((BLOCK, BLOCK), kind)
    window = pltpu.VMEM(((reach + 1) * per_dev, 2, BLOCK, head_dim), kind)
    hbm = pl.BlockSpec(memory_space=pltpu.HBM)
    return pl.pallas_call(
        functools.partial(fused_kernel, size, kv_heads, relayed, dims),
        out_shape=jax.ShapeDtypeStruct((rows_dev, q_heads * head_dim), kind),
        in_specs=[hbm] * 7,
        out_specs=hbm,
        scratch_shapes=[
            pltpu.SMEM(vert_blocks.shape, jnp.int32),
            pltpu.SMEM(vert_count.shape, jnp.int32),
            pltpu.SMEM(slash_offsets.shape, jnp.int32),
            pltpu.SMEM(slash_count.shape, jnp.int32),
            pltpu.VMEM(keys.shape, kind),
            pltpu.VMEM(values.shape, kind),
            pltpu.VMEM(queries.shape, kind),
            pltpu.VMEM((rows_dev, q_heads * head_dim), kind),
            pltpu.VMEM((kv_heads, per_dev, 2, BLOCK, head_dim), kind),
            pltpu.VMEM((rows_dev, q_heads * head_dim), kind),
            columns,
            pltpu.VMEM((landed_rows, head_dim), kind),
            columns,
            pltpu.VMEM((relayed, per_dev, 2, BLOCK, head_dim), kind),
            square,
            square,
        ]
        + [window] * kv_heads
        + [dma((7,)), dma((kv_heads,))]
        + [dma((CHUNKS,))] * 6
        + [dma((CHUNKS, length))] * 6
        + [dma((kv_heads,))] * 4
        + [dma((relayed,))] * 2,
        compiler_params=pltpu.CompilerParams(
            collective_id=0, has_side_effects=True, vmem_limit_bytes=56 * 1024 * 1024
        ),
        name="fused",
    )(vert_blocks, vert_count, slash_offsets, slash_count, keys, values, queries)


def local(
    query_states, key_states, value_states, vert_blocks, vert_count, slash_offsets, slash_count
):
    out = fused(
        key_states,
        value_states,
        query_states,
        vert_blocks.T,
        vert_count,
        slash_offsets.T,
        slash_count,
    )
    return out.reshape(query_states.shape)


def solution(mesh):
    in_specs = (
        P(("groups", "ctx"), None, None),
        P(("groups", "ctx"), None, None),
        P(("groups", "ctx"), None, None),
        P("groups", None),
        P("groups"),
        P("groups", None),
        P("groups"),
    )
    out_specs = P(("groups", "ctx"), None, None)
    return jax.shard_map(local, mesh=mesh, in_specs=in_specs, out_specs=out_specs, check_vma=False)
```

```python
import functools
import math

import jax
import jax.numpy as jnp
from jax import lax
from jax.experimental import pallas as pl
from jax.experimental.pallas import tpu as pltpu
from jax.sharding import PartitionSpec as P

BLOCK = 128
LARGEST_OFFSET = 8
MASKED = -1e30
CHUNKS = 2


def attend_head(head, dims, device, tables, q_ref, window, columns, diagonal, unit, out_ref):
    per_dev, reach, n_vert, n_slash, group_size, head_dim = dims
    vb_ref, vc_ref, so_ref, sc_ref = tables
    scale = math.log2(math.e) / math.sqrt(head_dim)
    n_tiles = n_vert + n_slash
    chunk = 2 if group_size % 2 == 0 else 1
    parts = group_size // chunk

    def one_block(block, carry):
        qblock = device * per_dev + block
        start = pl.multiple_of(block * BLOCK, BLOCK)
        own = reach * per_dev + block
        spots, usable = [own], []
        for s in range(1, n_slash):
            offset = so_ref[s, head]
            ok = (s < sc_ref[head]) & (offset <= qblock)
            for v in range(n_vert):
                ok = ok & ((v >= vc_ref[head]) | (vb_ref[v, head] != qblock - offset))
            usable.append(ok)
            spots.append(jnp.where(ok, own - offset, own))
        for v in range(n_vert):
            usable.append((v < vc_ref[head]) & (vb_ref[v, head] < qblock))
        keys = [window[spot, 0] for spot in spots]
        values = [window[spot, 1] for spot in spots]
        for v in range(n_vert):
            row = (head * n_vert + v) * 2 * BLOCK
            keys.append(columns[row : row + BLOCK, :])
            values.append(columns[row + BLOCK : row + 2 * BLOCK, :])
        masks = [diagonal[...]]
        for ok in usable:
            fill = jnp.where(ok, 0.0, MASKED).astype(jnp.float32)
            masks.append(jnp.full((BLOCK, BLOCK), fill, jnp.float32).astype(jnp.bfloat16))
        keys = jnp.concatenate(
            [jnp.concatenate(keys, axis=0), jnp.concatenate(masks, axis=0)], axis=1
        )
        values = jnp.concatenate(values, axis=0)

        def scores_of(part):
            queries = []
            for h in range(part * chunk, (part + 1) * chunk):
                lane = (head * group_size + h) * head_dim
                rows = q_ref[pl.ds(start, BLOCK), lane : lane + head_dim]
                queries.append(jnp.concatenate([rows, unit[...]], axis=1))
            tile = lax.dot_general(
                jnp.concatenate(queries, axis=0), keys, (((1,), (1,)), ((), ())),
                preferred_element_type=jnp.float32,
            )
            return [tile[:, i * BLOCK : (i + 1) * BLOCK] for i in range(n_tiles)]

        def top_of(scores):
            return jnp.max(functools.reduce(jnp.maximum, scores), axis=1, keepdims=True)

        def sums_of(scores, top):
            powers = [jnp.exp2((tile - top) * scale) for tile in scores]
            total = jnp.sum(functools.reduce(jnp.add, powers), axis=1, keepdims=True)
            weights = jnp.concatenate([p.astype(jnp.bfloat16) for p in powers], axis=1)
            return jnp.dot(weights, values, preferred_element_type=jnp.float32), total

        def store(part, sums):
            result = (sums[0] / sums[1]).astype(jnp.bfloat16)
            for i in range(chunk):
                lane = (head * group_size + part * chunk + i) * head_dim
                out_ref[pl.ds(start, BLOCK), lane : lane + head_dim] = result[
                    i * BLOCK : (i + 1) * BLOCK
                ]

        scores = scores_of(0)
        top = top_of(scores)
        last = None
        for part in range(parts):
            following = scores_of(part + 1) if part + 1 < parts else None
            sums = sums_of(scores, top)
            if following is not None:
                top = top_of(following)
            if last is not None:
                store(part - 1, last)
            scores, last = following, sums
        store(parts - 1, last)
        return carry

    lax.fori_loop(0, per_dev, one_block, 0, unroll=2 if per_dev % 2 == 0 else 1)


def fused_kernel(
    size, kv_heads, relayed, dims,
    vb_hbm, vc_hbm, so_hbm, sc_hbm, k_hbm, v_hbm, q_hbm, out_hbm,
    vb_ref, vc_ref, so_ref, sc_ref, k_ref, v_ref, q_ref, out_ref, own_ref, qs_ref, acc, landed, full, stage, diagonal, unit, *scratch,
):
    per_dev, reach, n_vert, n_slash, group_size, head_dim = dims
    windows = scratch[:kv_heads]
    (
        load_sem, out_sem, core_send, core_recv, grow_send, grow_recv, swap_send, swap_recv,
        up_recv, down_recv, line_send, spread_recv, above_send, below_send,
        far_send, far_recv, near_send, near_recv, pass_send, pass_recv,
    ) = scratch[kv_heads:]
    tables = (vb_ref, vc_ref, so_ref, sc_ref)
    device = lax.axis_index("ctx")
    odd = lax.rem(device, 2)
    side = lax.rem(device // 2, 2)
    line = device // 4
    length = size // 4
    direct = kv_heads - relayed
    last = size - 1

    def remote(src, dst, send, recv, target):
        return pltpu.make_async_remote_copy(
            src_ref=src, dst_ref=dst, send_sem=send, recv_sem=recv,
            device_id={"ctx": target}, device_id_type=pl.DeviceIdType.MESH,
        )

    loads = [
        pltpu.make_async_copy(src, dst, load_sem.at[i])
        for i, (src, dst) in enumerate((
            (k_hbm, k_ref), (v_hbm, v_ref), (vb_hbm, vb_ref), (vc_hbm, vc_ref),
            (so_hbm, so_ref), (sc_hbm, sc_ref), (q_hbm, q_ref),
        ))
    ]
    for load in loads:
        load.start()

    sends_far = device + reach < size
    gets_far = device >= reach
    crossing = (side == 1) & sends_far
    passes = (side == 0) & (device + 2 * reach < size)
    gets_passed = (side == 0) & gets_far
    partner = device + 1 - 2 * odd
    across = device ^ 2
    above = jnp.minimum(device + 4, last)
    below = jnp.maximum(device - 4, 0)
    has_above = line < length - 1
    has_below = line > 0

    barrier = pltpu.get_barrier_semaphore()
    greeted = (
        (has_above, above), (has_below, below),
        (crossing, device + reach), (gets_passed, device - reach),
    )

    def greet(target):
        pl.semaphore_signal(
            barrier, inc=1, device_id={"ctx": target}, device_id_type=pl.DeviceIdType.MESH
        )

    greet(partner)
    greet(across)
    arrivals = jnp.int32(2)
    for condition, target in greeted:
        @pl.when(condition)
        def _(target=target):
            greet(target)

        arrivals = arrivals + condition.astype(jnp.int32)

    rows_i = lax.broadcasted_iota(jnp.int32, (BLOCK, BLOCK), 0)
    cols_i = lax.broadcasted_iota(jnp.int32, (BLOCK, BLOCK), 1)
    diagonal[...] = jnp.where(cols_i >= rows_i, 0.0, MASKED).astype(jnp.bfloat16)
    unit[...] = jnp.where(rows_i == cols_i, 1.0, 0.0).astype(jnp.bfloat16)

    def own_block(block, carry):
        rows = pl.ds(pl.multiple_of(block * BLOCK, BLOCK), BLOCK)
        for kv, ref in enumerate((k_ref, v_ref)):
            for head in range(kv_heads):
                tile = ref[rows, head, :]
                own_ref[head, block, kv] = tile
                windows[head][reach * per_dev + block, kv] = tile
        return carry

    with jax.named_scope("loads"):
        for load in loads[:-1]:
            load.wait()
    with jax.named_scope("own"):
        lax.fori_loop(0, per_dev, own_block, 0)

    def one_head(head, carry):
        for v in range(n_vert):
            at = vb_ref[v, head] - device * per_dev
            mine = (v < vc_ref[head]) & (at >= 0) & (at < per_dev)
            at = jnp.clip(at, 0, per_dev - 1)
            for kv in range(2):
                tile = own_ref[head, at, kv].astype(jnp.float32)
                row = pl.multiple_of(((head * n_vert + v) * 2 + kv) * BLOCK, BLOCK)
                acc[pl.ds(row, BLOCK), :] = jnp.where(mine, tile, 0.0).astype(jnp.bfloat16)
        return carry

    with jax.named_scope("terms"):
        lax.fori_loop(0, kv_heads, one_head, 0)
    with jax.named_scope("entry"):
        pl.semaphore_wait(barrier, arrivals)

    def place(head, where):
        return windows[head].at[pl.ds(where * per_dev, per_dev)]

    def far_copy(head):
        target = jnp.minimum(device + reach, last)
        return remote(own_ref.at[head], place(head, 0), far_send.at[head], far_recv.at[head], target)

    def stage_copy(head):
        slot = stage.at[head - direct]
        target = jnp.maximum(device - reach, 0)
        return remote(own_ref.at[head], slot, far_send.at[head], pass_recv.at[head - direct], target)

    def pass_copy(head):
        slot = stage.at[head - direct]
        return remote(
            slot, place(head, 0), pass_send.at[head - direct], far_recv.at[head], above
        )

    def near_copy(head):
        return remote(
            own_ref.at[head], place(head, 1), near_send.at[head], near_recv.at[head], partner
        )

    def relay_copy(head):
        return remote(
            place(head, 0), place(head, 1), near_send.at[head], near_recv.at[head], partner
        )

    def start_far(condition, heads):
        @pl.when(condition)
        def _():
            for head in heads:
                far_copy(head).start()

    def pass_on(condition, heads):
        @pl.when(passes & condition)
        def _():
            for head in heads:
                with jax.named_scope(f"stage#h={head}"):
                    stage_copy(head).wait_recv()
                pass_copy(head).start()

    chunk_rows = kv_heads * n_vert * 2 * BLOCK // CHUNKS
    half = chunk_rows // 2
    piece = half // length
    chunks = range(CHUNKS)

    def kept(c):
        return c * chunk_rows + odd * half

    def part(c, d):
        return pl.ds(pl.multiple_of(kept(c) + d * piece, 16), piece)

    def spot(c, d, way):
        return pl.ds(pl.multiple_of(((c * length + d) * 2 + way) * piece, 16), piece)

    def add(dst, at, landing, rows):
        step = min(rows, 256)

        def body(i, carry):
            here = pl.ds(pl.multiple_of(at + i * step, 16), step)
            there = pl.ds(pl.multiple_of(landing + i * step, 16), step)
            dst[here, :] = acc[here, :] + landed[there, :]
            return carry

        lax.fori_loop(0, rows // step, body, 0)

    def core_copy(c):
        given = pl.multiple_of(c * chunk_rows + (1 - odd) * half, 16)
        return remote(
            acc.at[pl.ds(given, half)], landed.at[pl.ds(landed_core + c * half, half)],
            core_send.at[c], core_recv.at[c], partner,
        )

    landed_core = CHUNKS * length * 2 * piece
    landed_swap = landed_core + CHUNKS * half

    def line_copy(c, d, way):
        recv = up_recv if way == 0 else down_recv
        target = above if way == 0 else below
        return remote(
            acc.at[part(c, d)], landed.at[spot(c, d, way)],
            line_send.at[c, d], recv.at[c, d], target,
        )

    def take(c, d, way):
        line_copy(c, d, way).wait_recv()
        add(acc, kept(c) + d * piece, ((c * length + d) * 2 + way) * piece, piece)

    def fold_up(c):
        for d in range(length - 1, 0, -1):
            @pl.when(line < d)
            def _(d=d):
                @pl.when(has_below)
                def _():
                    take(c, d, 0)

                line_copy(c, d, 0).start()

    def fold_down(c):
        for d in range(length - 1):
            @pl.when(line > d)
            def _(d=d):
                @pl.when(has_above)
                def _():
                    take(c, d, 1)

                line_copy(c, d, 1).start()

    lower = 2 * line < length

    def fold_line(c):
        @pl.when(lower)
        def _():
            fold_up(c)
            fold_down(c)

        @pl.when(jnp.logical_not(lower))
        def _():
            fold_down(c)
            fold_up(c)

    def finish_line(c):
        @pl.when(has_below)
        def _():
            take(c, line, 0)

        @pl.when(has_above)
        def _():
            take(c, line, 1)

    def swap_copy(c):
        return remote(
            acc.at[part(c, line)], landed.at[pl.ds(landed_swap + c * piece, piece)],
            swap_send.at[c], swap_recv.at[c], across,
        )

    def spread_copy(c, d, way):
        send = above_send if way == 0 else below_send
        target = above if way == 0 else below
        return remote(
            full.at[part(c, d)], full.at[part(c, d)], send.at[c, d], spread_recv.at[c, d], target
        )

    def spread_own(c):
        swap_copy(c).wait_recv()
        add(full, kept(c) + line * piece, landed_swap + c * piece, piece)

        @pl.when(has_above)
        def _():
            spread_copy(c, line, 0).start()

        @pl.when(has_below)
        def _():
            spread_copy(c, line, 1).start()

    def spread_rest(c):
        for k in range(1, length):
            for way, d, found in ((0, line - k, line >= k), (1, line + k, line + k < length)):
                @pl.when(found)
                def _(way=way, d=d):
                    spread_copy(c, d, way).wait_recv()

                    @pl.when(has_above if way == 0 else has_below)
                    def _():
                        spread_copy(c, d, way).start()

    def grow_copy(c):
        rows = pl.ds(pl.multiple_of(kept(c), 16), half)
        return remote(full.at[rows], full.at[rows], grow_send.at[c], grow_recv.at[c], partner)

    early = kv_heads // 4
    middle = has_above & has_below
    edge = jnp.logical_not(middle)

    def stage_on(heads):
        @pl.when(crossing)
        def _():
            for head in heads:
                stage_copy(head).start()

    for c in chunks:
        core_copy(c).start()
    start_far(side == 0, range(early))
    stage_on(range(direct, direct + 2))
    start_far(crossing & (line == length - 2) & (line > 0), range(2))

    @pl.when(odd == 0)
    def _():
        for head in range(kv_heads):
            near_copy(head).start()

    for c in chunks:
        with jax.named_scope(f"core#c={c}"):
            core_copy(c).wait_recv()
            add(acc, kept(c), landed_core + c * half, half)
        if c == 0:
            with jax.named_scope(f"fold#c={c}"):
                fold_line(c)

    def queries(block, carry):
        rows = pl.ds(pl.multiple_of(block * BLOCK, BLOCK), BLOCK)
        for h in range(kv_heads * group_size):
            qs_ref[rows, h * head_dim : (h + 1) * head_dim] = q_ref[rows, h, :]
        return carry

    @pl.when(edge)
    def _():
        with jax.named_scope("fold_edge#c=1"):
            fold_line(1)

    loads[-1].wait()

    @pl.when(edge)
    def _():
        with jax.named_scope("queries_edge"):
            lax.fori_loop(0, per_dev, queries, 0)

    with jax.named_scope("finish#c=0"):
        finish_line(0)
    swap_copy(0).start()
    stage_on(range(direct + 2, direct + 3))
    pass_on((line == length - 2) & (line > 0), range(direct, direct + 2))

    @pl.when(middle)
    def _():
        with jax.named_scope("fold_mid#c=1"):
            fold_line(1)

    with jax.named_scope("swap#c=0"):
        spread_own(0)
    with jax.named_scope("finish#c=1"):
        finish_line(1)
    swap_copy(1).start()
    start_far(side == 0, range(early, kv_heads))
    stage_on(range(direct + 3, kv_heads))

    @pl.when(middle)
    def _():
        with jax.named_scope("queries#p=0"):
            lax.fori_loop(0, per_dev // 2, queries, 0)

    with jax.named_scope("swap#c=1"):
        spread_own(1)
    late = (line != length - 2) | (line == 0)
    start_far(crossing & (line == 0), range(2))
    pass_on(line == 0, range(direct, direct + 2))

    @pl.when(edge & gets_far & (odd == 1))
    def _():
        for head in range(2):
            far_copy(head).wait_recv()
            relay_copy(head).start()

    with jax.named_scope("spread#c=0"):
        spread_rest(0)
    grow_copy(0).start()
    start_far(crossing & late & (line > 0), range(1))
    pass_on(late & (line > 0), range(direct, direct + 1))

    @pl.when(middle)
    def _():
        with jax.named_scope("queries#p=1"):
            lax.fori_loop(per_dev // 2, per_dev, queries, 0)


    heads_chunk = kv_heads // CHUNKS

    def get_head(head, handed=False):
        with jax.named_scope(f"far#h={head}"):
            @pl.when(gets_far & (odd == 0) if handed else gets_far)
            def _():
                far_copy(head).wait_recv()

                if not handed:
                    @pl.when(odd == 1)
                    def _():
                        relay_copy(head).start()

        with jax.named_scope(f"near#h={head}"):
            @pl.when((odd == 1) | gets_far)
            def _():
                near_copy(head).wait_recv()

    def out_copy(head):
        lanes = pl.ds(head * group_size * head_dim, group_size * head_dim)
        return pltpu.make_async_copy(out_ref.at[:, lanes], out_hbm.at[:, lanes], out_sem.at[head])

    def do_head(head):
        with jax.named_scope(f"attend#h={head}"):
            attend_head(
                head, dims, device, tables, qs_ref, windows[head], full, diagonal, unit, out_ref
            )
        out_copy(head).start()

    def do_first(heads, handed):
        with jax.named_scope("grow#c=0"):
            grow_copy(0).wait_recv()
        for head in heads:
            get_head(head, handed)
            do_head(head)

    @pl.when(edge)
    def _():
        do_first(range(2), True)

    with jax.named_scope("spread#c=1"):
        spread_rest(1)
    grow_copy(1).start()
    start_far(crossing & late & (line > 0), range(1, 2))
    pass_on(late & (line > 0), range(direct + 1, direct + 2))
    start_far(crossing, range(2, direct))

    @pl.when(middle)
    def _():
        do_first(range(1), False)

    with jax.named_scope("grow#c=1"):
        grow_copy(1).wait_recv()
    order = [h for i in range(kv_heads) for h in (i, direct + i) if i < direct and h < kv_heads]
    order = [h for h in order if h > 1]
    for step, head in enumerate(order):
        get_head(head)
        do_head(head)
        if step == 0:
            @pl.when(middle)
            def _():
                get_head(1)
                do_head(1)

        if direct + 2 + step < kv_heads:
            pass_on(line >= 0, range(direct + 2 + step, direct + 3 + step))

    for head in range(kv_heads):
        out_copy(head).wait()

    @pl.when(sends_far)
    def _():
        for head in range(kv_heads):
            far_copy(head).wait_send()

    @pl.when((odd == 0) | gets_far)
    def _():
        for head in range(kv_heads):
            near_copy(head).wait_send()

    @pl.when(passes)
    def _():
        for head in range(direct, kv_heads):
            pass_copy(head).wait_send()

    for c in chunks:
        core_copy(c).wait_send()
        swap_copy(c).wait_send()
        grow_copy(c).wait_send()
        for d in range(length):
            @pl.when(line != d)
            def _(d=d):
                line_copy(c, d, 0).wait_send()

            @pl.when((line >= d) & has_above)
            def _(d=d):
                spread_copy(c, d, 0).wait_send()

            @pl.when((line <= d) & has_below)
            def _(d=d):
                spread_copy(c, d, 1).wait_send()


def fused(keys, values, queries, vert_blocks, vert_count, slash_offsets, slash_count):
    size = lax.axis_size("ctx")
    rows_dev, kv_heads, head_dim = keys.shape
    q_heads = queries.shape[1]
    per_dev = rows_dev // BLOCK
    n_vert = vert_blocks.shape[0]
    n_slash = slash_offsets.shape[0]
    reach = -(-LARGEST_OFFSET // per_dev)
    relayed = kv_heads // 2
    length = size // 4
    dims = (per_dev, reach, n_vert, n_slash, q_heads // kv_heads, head_dim)
    dma = pltpu.SemaphoreType.DMA
    kind = keys.dtype
    column_rows = kv_heads * n_vert * 2 * BLOCK
    columns = pltpu.VMEM((column_rows, head_dim), kind)
    landed_rows = column_rows + column_rows // 2 + column_rows // 2 // length
    square = pltpu.VMEM((BLOCK, BLOCK), kind)
    window = pltpu.VMEM(((reach + 1) * per_dev, 2, BLOCK, head_dim), kind)
    hbm = pl.BlockSpec(memory_space=pltpu.HBM)
    return pl.pallas_call(
        functools.partial(fused_kernel, size, kv_heads, relayed, dims),
        out_shape=jax.ShapeDtypeStruct((rows_dev, q_heads * head_dim), kind),
        in_specs=[hbm] * 7,
        out_specs=hbm,
        scratch_shapes=[
            pltpu.SMEM(vert_blocks.shape, jnp.int32),
            pltpu.SMEM(vert_count.shape, jnp.int32),
            pltpu.SMEM(slash_offsets.shape, jnp.int32),
            pltpu.SMEM(slash_count.shape, jnp.int32),
            pltpu.VMEM(keys.shape, kind),
            pltpu.VMEM(values.shape, kind),
            pltpu.VMEM(queries.shape, kind),
            pltpu.VMEM((rows_dev, q_heads * head_dim), kind),
            pltpu.VMEM((kv_heads, per_dev, 2, BLOCK, head_dim), kind),
            pltpu.VMEM((rows_dev, q_heads * head_dim), kind),
            columns,
            pltpu.VMEM((landed_rows, head_dim), kind),
            columns,
            pltpu.VMEM((relayed, per_dev, 2, BLOCK, head_dim), kind),
            square,
            square,
        ]
        + [window] * kv_heads
        + [dma((7,)), dma((kv_heads,))]
        + [dma((CHUNKS,))] * 6
        + [dma((CHUNKS, length))] * 6
        + [dma((kv_heads,))] * 4
        + [dma((relayed,))] * 2,
        compiler_params=pltpu.CompilerParams(
            collective_id=0, has_side_effects=True, vmem_limit_bytes=56 * 1024 * 1024
        ),
        name="fused",
    )(vert_blocks, vert_count, slash_offsets, slash_count, keys, values, queries)


def local(
    query_states, key_states, value_states, vert_blocks, vert_count, slash_offsets, slash_count
):
    out = fused(
        key_states,
        value_states,
        query_states,
        vert_blocks.T,
        vert_count,
        slash_offsets.T,
        slash_count,
    )
    return out.reshape(query_states.shape)


def solution(mesh):
    in_specs = (
        P(("groups", "ctx"), None, None),
        P(("groups", "ctx"), None, None),
        P(("groups", "ctx"), None, None),
        P("groups", None),
        P("groups"),
        P("groups", None),
        P("groups"),
    )
    out_specs = P(("groups", "ctx"), None, None)
    return jax.shard_map(local, mesh=mesh, in_specs=in_specs, out_specs=out_specs, check_vma=False)
```
